32 devices in a mesh: sec: 8 (over y, x, core), pan: 4 (over z).
Axes of the slice: x: 2, y: 2, z: 4, core: 2. Of those that a mesh axis runs over, the one named last changes fastest.
Arguments:
- wave_state: bfloat16 [8, 512, 512], P('sec', 'pan'), may hold values from -6 to 6
- right_blocks: bfloat16 [8, 16, 512, 512], P('sec', None, None, 'pan'), may hold values from -0.25 to 0.25
- left_blocks: bfloat16 [576, 512, 512], P('sec', 'pan'), may hold values from -0.125 to 0.125
- coupling: bfloat16 [576], P('sec'), may hold values from -1 to 1
- channel_term: int32 [576], P('sec'), may hold values from 0 to 15
- channel_out: int32 [576], P('sec'), may hold values from 0 to 7, as said below
- sector_dims: int32 [8], P('sec'), may hold values from 128 to 512
Outputs:
- applied: float32 [8, 512, 512], P('sec', 'pan')
The draws below stay inside these ranges and needn't reach their ends.
Inputs may be any that keep to these rules, and one draw needn't show every extreme that they name: `channel_out`: channel c ends in a sector at most two away from the sector c // 72 that it starts from.
All inputs are finite; a program needn't handle non-finite values.
Results may differ from the reference program's by a relative error of at most 0.0041.
Values may be sent and summed in bfloat16 or wider, within the bound.
A program may use at most 128 MiB of HBM per device.

```python
import jax
import jax.numpy as jnp
from jax import lax

DB = 512
NW = 16
CH_DEV = 72
SECTORS = 8
CHANNELS = 576


def draw_channel_out(key, part):
    chan_total = CH_DEV * SECTORS
    source = jnp.arange(chan_total, dtype=jnp.int32) // CH_DEV
    offset = jax.random.randint(key, (chan_total,), -2, 3, dtype=jnp.int32)
    return jnp.clip(source + offset, 0, SECTORS - 1).astype(jnp.int32)


def place_ends(drawn, stream_key, low, largest):
    longest = drawn.shape.index(max(drawn.shape))
    spots = []
    for shift in (0, 1):
        where = [jax.random.randint(jax.random.fold_in(stream_key, axis), (), 0, length) for axis, length in enumerate(drawn.shape)]
        where[longest] = (where[longest] + shift) % drawn.shape[longest]
        spots.append(tuple(where))
    return drawn.at[spots[0]].set(low).at[spots[1]].set(largest)


def block_scale(own_key, shape, pieces, smallest, largest):
    factor_of = 1.0
    for position, shards_of in pieces:
        draws = jax.random.uniform(jax.random.fold_in(jax.random.fold_in(own_key, 6), position), (shards_of,), jnp.float32, smallest / len(pieces), largest / len(pieces))
        factor_of = factor_of * jnp.repeat(jnp.exp(draws), shape[position] // shards_of).reshape((-1,) + (1,) * (len(shape) - 1 - position))
    return factor_of


def bell_draw(rng, extent, spread, reach, shards=(), kind=jnp.bfloat16):
    gain = block_scale(rng, extent, shards, -0.22, 0.18) if shards else 1.0
    drawn = jax.random.normal(rng, extent, jnp.float32) * spread * gain
    return jnp.minimum(jnp.maximum(drawn, -reach), reach).astype(kind)


def setup_inputs(seed: int = 0) -> dict:
    streams_of = jax.random.split(jax.random.key(seed), 8)
    return {
        "wave_state": bell_draw(streams_of[0], (SECTORS, DB, DB), 1.0, 6.0, ((0, 8), (1, 4))),
        "right_blocks": bell_draw(streams_of[1], (SECTORS, NW, DB, DB), DB ** -0.5, 0.25, ((0, 8), (3, 4))),
        "left_blocks": bell_draw(streams_of[2], (CHANNELS, DB, DB), (4 * DB) ** -0.5, 0.125, ((0, 8), (1, 4))),
        "coupling": jnp.clip(jax.random.uniform(streams_of[3], (CHANNELS,), jnp.float32, -1.0, 1.0) * block_scale(streams_of[3], (CHANNELS,), ((0, 8),), -0.4, 0.0), -1.0, 1.0).astype(jnp.bfloat16),
        "channel_term": place_ends(jax.random.randint(streams_of[4], (CHANNELS,), 0, NW), jax.random.fold_in(streams_of[4], 1), 0, NW - 1).astype(jnp.int32),
        "channel_out": draw_channel_out(jax.random.fold_in(streams_of[7], 71), 0),
        "sector_dims": place_ends(jax.random.randint(streams_of[6], (SECTORS,), DB // 4, DB + 1), jax.random.fold_in(streams_of[6], 1), DB // 4, DB).astype(jnp.int32),
    }


def reference(wave_state, right_blocks, left_blocks, coupling, channel_term, channel_out, sector_dims):
    indices = jnp.arange(DB, dtype=jnp.int32)
    slot_ids = jnp.arange(5, dtype=jnp.int32)
    term_ids = jnp.arange(NW, dtype=jnp.int32)

    def visit_sector(totals, sector):
        live_dim = sector_dims[sector]
        inside = (indices[:, None] < live_dim) & (indices[None, :] < live_dim)
        masked = jnp.where(inside, wave_state[sector], jnp.zeros((), jnp.bfloat16))
        terms_here = jnp.einsum("ik,wkq->wiq", masked.astype(jnp.float32), right_blocks[sector].astype(jnp.float32)).astype(jnp.bfloat16)
        first_chan = (sector * CH_DEV).astype(jnp.int32)
        left_part = lax.dynamic_slice_in_dim(left_blocks, first_chan, CH_DEV, 0)
        coef_part = lax.dynamic_slice_in_dim(coupling, first_chan, CH_DEV, 0)
        kind_part = lax.dynamic_slice_in_dim(channel_term, first_chan, CH_DEV, 0)
        targets = lax.dynamic_slice_in_dim(channel_out, first_chan, CH_DEV, 0)
        slot_index = targets - sector + 2
        chosen = (slot_index[None, None, :] == slot_ids[:, None, None]) & (kind_part[None, None, :] == term_ids[None, :, None])
        weights = jnp.where(chosen, coef_part[None, None, :], jnp.zeros((), jnp.bfloat16)).reshape(5 * NW, CH_DEV)
        combined = jnp.dot(weights, left_part.reshape(CH_DEV, DB * DB), preferred_element_type=jnp.float32)
        combined = combined.astype(jnp.bfloat16).reshape(5, NW, DB, DB)
        partial_value = jnp.einsum("jwri,wiq->jrq", combined.astype(jnp.float32), terms_here.astype(jnp.float32))
        window = lax.dynamic_slice_in_dim(totals, sector, 5, 0)
        totals = lax.dynamic_update_slice_in_dim(totals, window + partial_value, sector, 0)
        return totals, None

    start_totals = jnp.zeros((SECTORS + 4, DB, DB), jnp.float32)
    totals, _ = lax.scan(visit_sector, start_totals, jnp.arange(SECTORS, dtype=jnp.int32))
    summed = totals[2:SECTORS + 2]
    limits = sector_dims[:, None, None]
    kept_mask = (indices[None, :, None] < limits) & (indices[None, None, :] < limits)
    return jnp.where(kept_mask, summed, jnp.zeros((), jnp.float32))
```

```python
import functools

import jax
import jax.numpy as jnp
from jax import lax
from jax.experimental import pallas as pl
from jax.experimental.pallas import tpu as pltpu
from jax.sharding import PartitionSpec as P

OFFSETS = (-2, -1, 1, 2)
END_SLOTS = (0, 1, 3, 4, 2)
F32 = jnp.float32
BF16 = jnp.bfloat16


def combine_kernel(cell_ref, coef_ref, left_ref, out_ref, acc_ref):
    acc_ref[...] = jnp.zeros_like(acc_ref)

    @pl.loop(0, left_ref.shape[0])
    def _(channel):
        cell = cell_ref[channel]
        acc_ref[cell] += left_ref[channel].astype(F32) * coef_ref[channel]

    @pl.loop(0, out_ref.shape[0])
    def _(cell):
        out_ref[cell] = acc_ref[cell].astype(BF16)


def combine(cells, coefs, left_blocks, cell_count):
    channels, rows, width = left_blocks.shape
    step = min(rows, 32)
    return pl.pallas_call(
        combine_kernel,
        grid=(rows // step,),
        in_specs=[
            pl.BlockSpec(memory_space=pltpu.SMEM),
            pl.BlockSpec(memory_space=pltpu.SMEM),
            pl.BlockSpec((channels, step, width), lambda i: (0, i, 0)),
        ],
        out_specs=pl.BlockSpec((cell_count, step, width), lambda i: (0, i, 0)),
        out_shape=jax.ShapeDtypeStruct((cell_count, rows, width), BF16),
        scratch_shapes=[pltpu.VMEM((cell_count, step, width), F32)],
        compiler_params=pltpu.CompilerParams(vmem_limit_bytes=48 * 2**20),
    )(cells, coefs, left_blocks)


def read_channels(slots, terms, sector, term, out_id, coef, coefs, kept, filled, table):
    count = term.shape[0]
    cells = slots * terms
    width = coefs.shape[1]
    cell = (term[...] * slots + out_id[...] - sector + 2).astype(F32)
    cell_row = jnp.broadcast_to(cell[None, :], (count, count))
    coef_row = jnp.broadcast_to(coef[...].astype(F32)[None, :], (count, count))
    down = lax.broadcasted_iota(jnp.int32, (count, count), 0)
    across = lax.broadcasted_iota(jnp.int32, (count, count), 1)

    def total(mask, values, axis):
        return jnp.sum(jnp.where(mask, values, 0.0), axis=axis, keepdims=True)

    cell_col = total(down == across, cell_row, 1)
    same = cell_col == cell_row
    precedes = (cell_col < cell_row) | (same & (down < across))
    follows = (cell_row < cell_col) | (same & (across < down))
    rank_row = total(precedes, 1.0, 0)
    rank_col = total(follows, 1.0, 1)
    again = jnp.where(total(same & (down < across), 1.0, 0) > 0, 1.0, 0.0)
    spot = rank_row == down.astype(F32)
    coefs[...] = jnp.broadcast_to(total(spot, coef_row, 1), (count, width))
    kept[...] = jnp.broadcast_to(
        total(spot, jnp.broadcast_to(again, (count, count)), 1), (count, width)
    )
    order = total(rank_col == across.astype(F32), down.astype(F32), 0)
    cell_ids = lax.broadcasted_iota(jnp.int32, (count, cells), 1).astype(F32)
    last = total(jnp.broadcast_to(cell_col, (count, cells)) <= cell_ids, 1.0, 0) - 1.0
    ids_down = lax.broadcasted_iota(jnp.int32, (cells, count), 0).astype(F32)
    held = total(ids_down == jnp.broadcast_to(cell[None, :], (cells, count)), 1.0, 1)
    filled[...] = jnp.broadcast_to(jnp.where(held > 0, 1.0, 0.0), (cells, width))
    table[0:1, 0:count] = order.astype(jnp.int32)
    table[1:2, 0:cells] = jnp.maximum(last, 0.0).astype(jnp.int32)


def line_kernel(
    sectors, moved, dims_ref, term_ref, out_id_ref, coef_ref, state_ref, right_ref, left_ref,
    out_ref,
    dims, term_ids, out_ids, coef, table, spots, coefs, kept, filled,
    left_all, running, summed,
    state_all, masked, gathered, comb, comb_end, kept_terms, acc, acc_end,
    stage, landed, stage_end, landed_end, back, back_landed,
    local_sems, state_send, state_recv, own_send, relay_send, right_recv,
    end_send, end_recv, part_send, part_recv, part_end_send, part_end_recv, back_sems,
):
    terms, width, cols = right_ref.shape
    rows = state_ref.shape[0]
    slots = comb.shape[1] // rows
    home = slots // 2
    me = lax.axis_index("pan")
    sector = lax.axis_index("sec")
    is_mid = (me == 1) | (me == 2)
    is_end = jnp.logical_not(is_mid)
    near_end = jnp.where(me <= 1, 0, 3)
    other_mid = jnp.where(me <= 1, 2, 1)
    far_end = 3 - near_end
    near_mid = jnp.where(me <= 1, 1, 2)

    def remote(src, dst, send, recv, where, axis="pan"):
        return pltpu.make_async_remote_copy(
            src_ref=src, dst_ref=dst, send_sem=send, recv_sem=recv,
            device_id={axis: where}, device_id_type=pl.DeviceIdType.MESH,
        )

    def state_own(way, where):
        return remote(state_ref, state_all.at[me], state_send.at[way], state_recv.at[me], where)

    def state_relay(way, owner, where):
        block = state_all.at[owner]
        return remote(block, block, state_send.at[way], state_recv.at[owner], where)

    def state_wait(owner):
        state_relay(0, owner, me).wait_recv()

    def own_copy(way, term, where):
        return remote(
            right_ref.at[term], gathered.at[me, term],
            own_send.at[way, term], right_recv.at[me, term], where,
        )

    def relay_copy(way, owner, term, where):
        block = gathered.at[owner, term]
        return remote(block, block, relay_send.at[way, term], right_recv.at[owner, term], where)

    def end_copy(slot, term, where):
        spot = pl.ds(pl.multiple_of(slot * rows, rows), rows)
        return remote(
            comb.at[term, spot], comb_end.at[slot, term],
            end_send.at[slot, term], end_recv.at[slot, term], where,
        )

    def arrived(owner, term):
        block = gathered.at[owner, term]
        remote(block, block, relay_send.at[0, term], right_recv.at[owner, term], me).wait_recv()

    def part_copy(index, owner):
        return remote(
            stage.at[index, owner], landed.at[index, owner],
            part_send.at[index, owner], part_recv.at[index, owner], sector + OFFSETS[index], "sec",
        )

    def part_end_copy(index):
        return remote(
            stage_end.at[index], landed_end.at[index],
            part_end_send.at[index], part_end_recv.at[index], sector + OFFSETS[index], "sec",
        )

    def back_copy(where):
        return remote(back, back_landed, back_sems.at[0], back_sems.at[1], where)

    def goes(index):
        target = sector + OFFSETS[index]
        return (target >= 0) & (target < sectors)

    def comes(index):
        source = sector - OFFSETS[index]
        return (source >= 0) & (source < sectors)

    barrier = pltpu.get_barrier_semaphore()

    def greet(axis, where):
        pl.semaphore_signal(
            barrier, inc=1, device_id={axis: where}, device_id_type=pl.DeviceIdType.MESH
        )

    greet("pan", jnp.where(is_mid, near_end, near_mid))

    @pl.when(is_mid)
    def _():
        greet("pan", other_mid)

    peers = jnp.where(is_mid, 2, 1)
    for index in range(4):
        peers = peers + goes(index).astype(jnp.int32)

        @pl.when(goes(index))
        def _():
            greet("sec", sector + OFFSETS[index])

    pl.semaphore_wait(barrier, peers)

    early = min(2, terms - moved)

    @pl.when(is_mid)
    def _():
        state_own(0, near_end).start()
        state_own(1, other_mid).start()

        @pl.loop(0, early)
        def _(term):
            own_copy(1, moved + term, near_end).start()
            own_copy(0, term, other_mid).start()

    @pl.when(is_end)
    def _():
        state_own(0, near_mid).start()

        @pl.loop(0, terms)
        def _(term):
            own_copy(0, term, near_mid).start()

    small = [
        pltpu.make_async_copy(dims_ref, dims, local_sems.at[0]),
        pltpu.make_async_copy(term_ref, term_ids, local_sems.at[1]),
        pltpu.make_async_copy(out_id_ref, out_ids, local_sems.at[2]),
        pltpu.make_async_copy(coef_ref, coef, local_sems.at[3]),
    ]
    large = [
        pltpu.make_async_copy(left_ref, left_all, local_sems.at[4]),
        pltpu.make_async_copy(state_ref, state_all.at[me], local_sems.at[5]),
        pltpu.make_async_copy(right_ref, gathered.at[me], local_sems.at[6]),
    ]
    for copy in small + large:
        copy.start()
    for copy in small:
        copy.wait()
    read_channels(slots, terms, sector, term_ids, out_ids, coef, coefs, kept, filled, table)
    spots_copy = pltpu.make_async_copy(table, spots, local_sems.at[7])
    spots_copy.start()
    acc[...] = jnp.zeros_like(acc)
    acc_end[...] = jnp.zeros_like(acc_end)
    running[...] = jnp.zeros_like(running)

    later = min(early + 3, terms - moved)

    @pl.when(is_mid)
    def _():
        state_wait(other_mid)
        state_relay(2, other_mid, near_end).start()
        state_wait(near_end)
        state_relay(3, near_end, other_mid).start()

        @pl.loop(early, later)
        def _(term):
            own_copy(1, moved + term, near_end).start()

        @pl.loop(early, terms)
        def _(term):
            own_copy(0, term, other_mid).start()

    spots_copy.wait()
    for copy in large:
        copy.wait()

    channels = left_all.shape[0]

    def inside(spot):
        return jnp.minimum(jnp.maximum(spot, 0), channels - 1)

    @pl.loop(0, channels)
    def _(step):
        row = pl.ds(step, 1)
        total = running[...] * kept[row, :] + left_all[inside(spots[0, step])].astype(F32) * coefs[row, :]
        running[...] = total
        summed[step] = total.astype(BF16)

    @pl.loop(0, terms)
    def _(term):
        for slot in range(slots):
            cell = term * slots + slot
            value = summed[inside(spots[1, cell])].astype(F32) * filled[pl.ds(cell, 1), :]
            comb[term, slot * rows:(slot + 1) * rows, :] = value.astype(BF16)

    @pl.when(is_mid)
    def _():
        state_wait(far_end)
        state_relay(4, far_end, near_end).start()

        @pl.loop(later, terms - moved)
        def _(term):
            own_copy(1, moved + term, near_end).start()

    @pl.when(is_end)
    def _():
        for slot in END_SLOTS:
            @pl.loop(0, moved)
            def _(term):
                end_copy(slot, term, near_mid).start()

        for owner in (near_mid, 3 - near_mid, 3 - me):
            state_wait(owner)

    live = dims[0]
    inside_col = lax.broadcasted_iota(jnp.int32, (rows, width), 1) < live
    for owner in range(4):
        row = lax.broadcasted_iota(jnp.int32, (rows, width), 0) + owner * rows
        masked[owner * rows:(owner + 1) * rows, :] = jnp.where(
            inside_col & (row < live), state_all[owner].astype(F32), 0.0
        ).astype(BF16)

    def multiply(owner, term, keep=False):
        block = jnp.dot(masked[...], gathered[owner, term], preferred_element_type=F32).astype(BF16)
        if keep:
            kept_terms[term, owner] = block
        acc[owner] += jnp.dot(comb[term], block, preferred_element_type=F32)

    def send_parts(owner):
        for index in range(4):
            slot = OFFSETS[index] + 2

            @pl.when(goes(index))
            def _():
                stage[index, owner] = acc[owner, slot * rows:(slot + 1) * rows, :].astype(BF16)
                part_copy(index, owner).start()

    def take_parts(owner):
        for index in range(4):
            @pl.when(comes(index))
            def _():
                part_copy(index, owner).wait_recv()
                acc[owner, home * rows:(home + 1) * rows, :] += landed[index, owner].astype(F32)

    def write_out(owner):
        for spot in range(4):
            @pl.when(owner == spot)
            def _():
                out_ref[:, spot * cols:(spot + 1) * cols] = acc[spot, home * rows:(home + 1) * rows, :]

    def end_slot(slot):
        @pl.loop(0, moved)
        def _(term):
            end_copy(slot, term, me).wait_recv()

            @pl.loop(0, 4)
            def _(owner):
                acc_end[slot, owner] += jnp.dot(
                    comb_end[slot, term], kept_terms[term, owner], preferred_element_type=F32
                )

    @pl.when(is_mid)
    def _():
        def first_pass(begin, end, keep):
            @pl.loop(begin, end)
            def _(term):
                arrived(other_mid, term)
                if not keep:
                    relay_copy(0, other_mid, term, near_end).start()
                arrived(near_end, term)
                relay_copy(1, near_end, term, other_mid).start()

                @pl.loop(0, 3)
                def _(which):
                    owner = jnp.where(which == 0, me, jnp.where(which == 1, other_mid, near_end))
                    multiply(owner, term, keep)

        first_pass(0, moved, True)
        first_pass(moved, terms, False)

        @pl.loop(0, 3)
        def _(which):
            send_parts(jnp.where(which == 0, me, jnp.where(which == 1, other_mid, near_end)))

        @pl.loop(0, moved)
        def _(term):
            arrived(far_end, term)
            multiply(far_end, term, True)

        @pl.loop(moved, terms)
        def _(term):
            arrived(far_end, term)
            relay_copy(2, far_end, term, near_end).start()
            multiply(far_end, term)

            for index in range(4):
                slot = OFFSETS[index] + 2

                @pl.when(term == turn_of(index, moved, terms))
                def _():
                    end_slot(slot)

                    @pl.when(goes(index))
                    def _():
                        stage_end[index] = acc_end[slot].astype(BF16)
                        part_end_copy(index).start()

        send_parts(far_end)
        end_slot(home)

        for index in range(4):
            @pl.when(comes(index))
            def _():
                part_end_copy(index).wait_recv()
                acc_end[home] += landed_end[index].astype(F32)

        back[...] = acc_end[home].astype(BF16)
        back_copy(near_end).start()

        @pl.loop(0, 4)
        def _(owner):
            take_parts(owner)
            write_out(owner)

    @pl.when(is_end)
    def _():
        turn = jnp.where(me == 0, 1, -1)

        @pl.loop(0, 4)
        def _(rank):
            owner = me + turn * rank

            @pl.loop(moved, terms)
            def _(term):
                @pl.when(rank > 0)
                def _():
                    arrived(owner, term)

                multiply(owner, term)

            send_parts(owner)

        @pl.loop(0, 4)
        def _(rank):
            take_parts(me + turn * rank)

        back_copy(me).wait_recv()
        acc[:, home * rows:(home + 1) * rows, :] += back_landed[...].astype(F32)

        @pl.loop(0, 4)
        def _(owner):
            write_out(owner)

    for index in range(4):
        @pl.when(goes(index))
        def _():
            @pl.loop(0, 4)
            def _(owner):
                part_copy(index, owner).wait_send()

            @pl.when(is_mid)
            def _():
                part_end_copy(index).wait_send()

    @pl.when(is_mid)
    def _():
        state_own(0, near_end).wait_send()
        state_own(1, other_mid).wait_send()
        state_relay(2, other_mid, near_end).wait_send()
        state_relay(3, near_end, other_mid).wait_send()
        state_relay(4, far_end, near_end).wait_send()

        @pl.loop(0, terms)
        def _(term):
            own_copy(0, term, other_mid).wait_send()
            relay_copy(1, near_end, term, other_mid).wait_send()

            @pl.when(term >= moved)
            def _():
                own_copy(1, term, near_end).wait_send()
                relay_copy(0, other_mid, term, near_end).wait_send()
                relay_copy(2, far_end, term, near_end).wait_send()

        back_copy(near_end).wait_send()

    @pl.when(is_end)
    def _():
        state_own(0, near_mid).wait_send()

        @pl.loop(0, terms)
        def _(term):
            own_copy(0, term, near_mid).wait_send()

        for slot in END_SLOTS:
            @pl.loop(0, moved)
            def _(term):
                end_copy(slot, term, near_mid).wait_send()


def turn_of(index, moved, terms):
    steps = terms - moved
    return moved + min(steps - 1, max(0, (steps * (4 * index - 2)) // 12))


def line_apply(sectors, slots, dims, channel_term, channel_out, coefs, state, right, left):
    terms, width, cols = right.shape
    rows = state.shape[0]
    channels = left.shape[0]
    cells = slots * terms
    moved = max(1, terms // 4)
    tall = slots * rows
    dma = pltpu.SemaphoreType.DMA
    any_space = pl.BlockSpec(memory_space=pl.ANY)
    return pl.pallas_call(
        functools.partial(line_kernel, sectors, moved),
        out_shape=jax.ShapeDtypeStruct((rows, width), F32),
        in_specs=[any_space] * 7,
        out_specs=pl.BlockSpec(memory_space=pltpu.VMEM),
        scratch_shapes=[
            pltpu.SMEM(dims.shape, jnp.int32),
            pltpu.VMEM((channels,), jnp.int32),
            pltpu.VMEM((channels,), jnp.int32),
            pltpu.VMEM((channels,), BF16),
            pltpu.VMEM((8, 128), jnp.int32),
            pltpu.SMEM((8, 128), jnp.int32),
            pltpu.VMEM((channels, width), F32),
            pltpu.VMEM((channels, width), F32),
            pltpu.VMEM((cells, width), F32),
            pltpu.VMEM(left.shape, BF16),
            pltpu.VMEM((rows, width), F32),
            pltpu.VMEM(left.shape, BF16),
            pltpu.VMEM((4, rows, width), BF16),
            pltpu.VMEM((width, width), BF16),
            pltpu.VMEM((4, terms, width, cols), BF16),
            pltpu.VMEM((terms, tall, width), BF16),
            pltpu.VMEM((slots, moved, rows, width), BF16),
            pltpu.VMEM((moved, 4, width, cols), BF16),
            pltpu.VMEM((4, tall, cols), F32),
            pltpu.VMEM((slots, 4, rows, cols), F32),
            pltpu.VMEM((4, 4, rows, cols), BF16),
            pltpu.VMEM((4, 4, rows, cols), BF16),
            pltpu.VMEM((4, 4, rows, cols), BF16),
            pltpu.VMEM((4, 4, rows, cols), BF16),
            pltpu.VMEM((4, rows, cols), BF16),
            pltpu.VMEM((4, rows, cols), BF16),
            dma((8,)), dma((5,)), dma((4,)),
            dma((2, terms)), dma((3, terms)), dma((4, terms)),
            dma((slots, moved)), dma((slots, moved)),
            dma((4, 4)), dma((4, 4)), dma((4,)), dma((4,)), dma((2,)),
        ],
        compiler_params=pltpu.CompilerParams(
            has_side_effects=True, collective_id=0, vmem_limit_bytes=60 * 2**20
        ),
    )(dims, channel_term, channel_out, coefs, state, right, left)


def passed_along(value, axis, steps):
    count = lax.axis_size(axis)
    first, last = (max(0, -steps), min(count, count - steps))
    return lax.ppermute(value, axis, [(source, source + steps) for source in range(first, last)])


def gathered_apply(sector, live_dim, wave, right, combined, rows, slots):
    width = wave.shape[1]
    terms = right.shape[0]
    whole_state = lax.all_gather(wave, "pan", axis=0, tiled=True)
    indices = lax.iota(jnp.int32, width)
    inside = (indices[:, None] < live_dim) & (indices[None, :] < live_dim)
    masked = jnp.where(inside, whole_state, jnp.zeros((), BF16))
    right_full = lax.all_gather(right, "pan", axis=2, tiled=True)
    term_full = jnp.einsum("ik,wkq->wiq", masked, right_full, preferred_element_type=F32).astype(BF16)
    parts = jnp.einsum(
        "wjri,wiq->jrq", combined.reshape(terms, slots, rows, width), term_full,
        preferred_element_type=F32,
    )
    collected = parts[2]
    for offset in OFFSETS:
        collected = collected + passed_along(parts[offset + 2], "sec", offset)
    return collected


def on_device(
    wave_state, right_blocks, left_blocks, coupling, channel_term, channel_out, sector_dims
):
    rows, width = wave_state.shape[1:]
    terms = right_blocks.shape[1]
    slots = 5
    sector = lax.axis_index("sec")
    live_dim = sector_dims[0]
    if lax.axis_size("pan") == 4 and right_blocks.shape[3] % 128 == 0:
        collected = line_apply(
            lax.axis_size("sec"), slots, sector_dims, channel_term, channel_out, coupling,
            wave_state[0], right_blocks[0], left_blocks,
        )
    else:
        cells = channel_term * slots + channel_out - sector + 2
        coefs = coupling.astype(F32)
        combined = combine(cells, coefs, left_blocks, terms * slots)
        collected = gathered_apply(
            sector, live_dim, wave_state[0], right_blocks[0], combined, rows, slots
        )
    indices = lax.iota(jnp.int32, width)
    row_ids = lax.axis_index("pan") * rows + lax.iota(jnp.int32, rows)
    kept_mask = (row_ids[:, None] < live_dim) & (indices[None, :] < live_dim)
    return jnp.where(kept_mask, collected, jnp.zeros((), F32))[None]


def solution(mesh):
    return jax.shard_map(
        on_device,
        mesh=mesh,
        in_specs=(
            P("sec", "pan", None),
            P("sec", None, None, "pan"),
            P("sec", "pan", None),
            P("sec"),
            P("sec"),
            P("sec"),
            P("sec"),
        ),
        out_specs=P("sec", "pan", None),
        check_vma=False,
    )
```

```python
import functools

import jax
import jax.numpy as jnp
from jax import lax
from jax.experimental import pallas as pl
from jax.experimental.pallas import tpu as pltpu
from jax.sharding import PartitionSpec as P

OFFSETS = (-2, -1, 1, 2)
END_SLOTS = (0, 1, 3, 4, 2)
F32 = jnp.float32
BF16 = jnp.bfloat16


def combine_kernel(cell_ref, coef_ref, left_ref, out_ref, acc_ref):
    acc_ref[...] = jnp.zeros_like(acc_ref)

    @pl.loop(0, left_ref.shape[0])
    def _(channel):
        cell = cell_ref[channel]
        acc_ref[cell] += left_ref[channel].astype(F32) * coef_ref[channel]

    @pl.loop(0, out_ref.shape[0])
    def _(cell):
        out_ref[cell] = acc_ref[cell].astype(BF16)


def combine(cells, coefs, left_blocks, cell_count):
    channels, rows, width = left_blocks.shape
    step = min(rows, 32)
    return pl.pallas_call(
        combine_kernel,
        grid=(rows // step,),
        in_specs=[
            pl.BlockSpec(memory_space=pltpu.SMEM),
            pl.BlockSpec(memory_space=pltpu.SMEM),
            pl.BlockSpec((channels, step, width), lambda i: (0, i, 0)),
        ],
        out_specs=pl.BlockSpec((cell_count, step, width), lambda i: (0, i, 0)),
        out_shape=jax.ShapeDtypeStruct((cell_count, rows, width), BF16),
        scratch_shapes=[pltpu.VMEM((cell_count, step, width), F32)],
        compiler_params=pltpu.CompilerParams(vmem_limit_bytes=48 * 2**20),
    )(cells, coefs, left_blocks)


def read_channels(slots, terms, sector, term, out_id, coef, coefs, kept, filled, table):
    count = term.shape[0]
    cells = slots * terms
    width = coefs.shape[1]
    cell = (term[...] * slots + out_id[...] - sector + 2).astype(F32)
    cell_row = jnp.broadcast_to(cell[None, :], (count, count))
    coef_row = jnp.broadcast_to(coef[...].astype(F32)[None, :], (count, count))
    down = lax.broadcasted_iota(jnp.int32, (count, count), 0)
    across = lax.broadcasted_iota(jnp.int32, (count, count), 1)

    def total(mask, values, axis):
        return jnp.sum(jnp.where(mask, values, 0.0), axis=axis, keepdims=True)

    cell_col = total(down == across, cell_row, 1)
    same = cell_col == cell_row
    precedes = (cell_col < cell_row) | (same & (down < across))
    follows = (cell_row < cell_col) | (same & (across < down))
    rank_row = total(precedes, 1.0, 0)
    rank_col = total(follows, 1.0, 1)
    again = jnp.where(total(same & (down < across), 1.0, 0) > 0, 1.0, 0.0)
    spot = rank_row == down.astype(F32)
    coefs[...] = jnp.broadcast_to(total(spot, coef_row, 1), (count, width))
    kept[...] = jnp.broadcast_to(
        total(spot, jnp.broadcast_to(again, (count, count)), 1), (count, width)
    )
    order = total(rank_col == across.astype(F32), down.astype(F32), 0)
    cell_ids = lax.broadcasted_iota(jnp.int32, (count, cells), 1).astype(F32)
    last = total(jnp.broadcast_to(cell_col, (count, cells)) <= cell_ids, 1.0, 0) - 1.0
    ids_down = lax.broadcasted_iota(jnp.int32, (cells, count), 0).astype(F32)
    held = total(ids_down == jnp.broadcast_to(cell[None, :], (cells, count)), 1.0, 1)
    filled[...] = jnp.broadcast_to(jnp.where(held > 0, 1.0, 0.0), (cells, width))
    table[0:1, 0:count] = order.astype(jnp.int32)
    table[1:2, 0:cells] = jnp.maximum(last, 0.0).astype(jnp.int32)


def line_kernel(
    sectors, moved, dims_ref, term_ref, out_id_ref, coef_ref, state_ref, right_ref, left_ref,
    out_ref,
    dims, term_ids, out_ids, coef, table, spots, coefs, kept, filled,
    left_all, running, summed,
    state_all, masked, gathered, comb, comb_end, kept_terms, acc, acc_end,
    stage, landed, stage_end, landed_end, back, back_landed,
    local_sems, state_send, state_recv, own_send, relay_send, right_recv,
    end_send, end_recv, part_send, part_recv, part_end_send, part_end_recv, back_sems,
):
    terms, width, cols = right_ref.shape
    rows = state_ref.shape[0]
    slots = comb.shape[1] // rows
    home = slots // 2
    me = lax.axis_index("pan")
    sector = lax.axis_index("sec")
    is_mid = (me == 1) | (me == 2)
    is_end = jnp.logical_not(is_mid)
    near_end = jnp.where(me <= 1, 0, 3)
    other_mid = jnp.where(me <= 1, 2, 1)
    far_end = 3 - near_end
    near_mid = jnp.where(me <= 1, 1, 2)

    def remote(src, dst, send, recv, where, axis="pan"):
        return pltpu.make_async_remote_copy(
            src_ref=src, dst_ref=dst, send_sem=send, recv_sem=recv,
            device_id={axis: where}, device_id_type=pl.DeviceIdType.MESH,
        )

    def state_own(way, where):
        return remote(state_ref, state_all.at[me], state_send.at[way], state_recv.at[me], where)

    def state_relay(way, owner, where):
        block = state_all.at[owner]
        return remote(block, block, state_send.at[way], state_recv.at[owner], where)

    def state_wait(owner):
        state_relay(0, owner, me).wait_recv()

    def own_copy(way, term, where):
        return remote(
            right_ref.at[term], gathered.at[me, term],
            own_send.at[way, term], right_recv.at[me, term], where,
        )

    def relay_copy(way, owner, term, where):
        block = gathered.at[owner, term]
        return remote(block, block, relay_send.at[way, term], right_recv.at[owner, term], where)

    def end_copy(slot, term, where):
        spot = pl.ds(pl.multiple_of(slot * rows, rows), rows)
        return remote(
            comb.at[term, spot], comb_end.at[slot, term],
            end_send.at[slot, term], end_recv.at[slot, term], where,
        )

    def arrived(owner, term):
        block = gathered.at[owner, term]
        remote(block, block, relay_send.at[0, term], right_recv.at[owner, term], me).wait_recv()

    def part_copy(index, owner):
        return remote(
            stage.at[index, owner], landed.at[index, owner],
            part_send.at[index, owner], part_recv.at[index, owner], sector + OFFSETS[index], "sec",
        )

    def part_end_copy(index):
        return remote(
            stage_end.at[index], landed_end.at[index],
            part_end_send.at[index], part_end_recv.at[index], sector + OFFSETS[index], "sec",
        )

    def back_copy(where):
        return remote(back, back_landed, back_sems.at[0], back_sems.at[1], where)

    def goes(index):
        target = sector + OFFSETS[index]
        return (target >= 0) & (target < sectors)

    def comes(index):
        source = sector - OFFSETS[index]
        return (source >= 0) & (source < sectors)

    barrier = pltpu.get_barrier_semaphore()

    def greet(axis, where):
        pl.semaphore_signal(
            barrier, inc=1, device_id={axis: where}, device_id_type=pl.DeviceIdType.MESH
        )

    greet("pan", jnp.where(is_mid, near_end, near_mid))

    @pl.when(is_mid)
    def _():
        greet("pan", other_mid)

    peers = jnp.where(is_mid, 2, 1)
    for index in range(4):
        peers = peers + goes(index).astype(jnp.int32)

        @pl.when(goes(index))
        def _():
            greet("sec", sector + OFFSETS[index])

    pl.semaphore_wait(barrier, peers)

    early = min(2, terms - moved)

    @pl.when(is_mid)
    def _():
        state_own(0, near_end).start()
        state_own(1, other_mid).start()

        @pl.loop(0, early)
        def _(term):
            own_copy(1, moved + term, near_end).start()
            own_copy(0, term, other_mid).start()

    @pl.when(is_end)
    def _():
        state_own(0, near_mid).start()

        @pl.loop(0, terms)
        def _(term):
            own_copy(0, term, near_mid).start()

    small = [
        pltpu.make_async_copy(dims_ref, dims, local_sems.at[0]),
        pltpu.make_async_copy(term_ref, term_ids, local_sems.at[1]),
        pltpu.make_async_copy(out_id_ref, out_ids, local_sems.at[2]),
        pltpu.make_async_copy(coef_ref, coef, local_sems.at[3]),
    ]
    large = [
        pltpu.make_async_copy(left_ref, left_all, local_sems.at[4]),
        pltpu.make_async_copy(state_ref, state_all.at[me], local_sems.at[5]),
        pltpu.make_async_copy(right_ref, gathered.at[me], local_sems.at[6]),
    ]
    for copy in small + large:
        copy.start()
    for copy in small:
        copy.wait()
    read_channels(slots, terms, sector, term_ids, out_ids, coef, coefs, kept, filled, table)
    spots_copy = pltpu.make_async_copy(table, spots, local_sems.at[7])
    spots_copy.start()
    acc[...] = jnp.zeros_like(acc)
    acc_end[...] = jnp.zeros_like(acc_end)
    running[...] = jnp.zeros_like(running)

    later = min(early + 3, terms - moved)

    @pl.when(is_mid)
    def _():
        state_wait(other_mid)
        state_relay(2, other_mid, near_end).start()
        state_wait(near_end)
        state_relay(3, near_end, other_mid).start()

        @pl.loop(early, later)
        def _(term):
            own_copy(1, moved + term, near_end).start()

        @pl.loop(early, terms)
        def _(term):
            own_copy(0, term, other_mid).start()

    spots_copy.wait()
    for copy in large:
        copy.wait()

    channels = left_all.shape[0]

    def inside(spot):
        return jnp.minimum(jnp.maximum(spot, 0), channels - 1)

    @pl.loop(0, channels)
    def _(step):
        row = pl.ds(step, 1)
        total = running[...] * kept[row, :] + left_all[inside(spots[0, step])].astype(F32) * coefs[row, :]
        running[...] = total
        summed[step] = total.astype(BF16)

    @pl.loop(0, terms)
    def _(term):
        for slot in range(slots):
            cell = term * slots + slot
            value = summed[inside(spots[1, cell])].astype(F32) * filled[pl.ds(cell, 1), :]
            comb[term, slot * rows:(slot + 1) * rows, :] = value.astype(BF16)

    @pl.when(is_mid)
    def _():
        state_wait(far_end)
        state_relay(4, far_end, near_end).start()

        @pl.loop(later, terms - moved)
        def _(term):
            own_copy(1, moved + term, near_end).start()

    @pl.when(is_end)
    def _():
        for slot in END_SLOTS:
            @pl.loop(0, moved)
            def _(term):
                end_copy(slot, term, near_mid).start()

        for owner in (near_mid, 3 - near_mid, 3 - me):
            state_wait(owner)

    live = dims[0]
    inside_col = lax.broadcasted_iota(jnp.int32, (rows, width), 1) < live
    for owner in range(4):
        row = lax.broadcasted_iota(jnp.int32, (rows, width), 0) + owner * rows
        masked[owner * rows:(owner + 1) * rows, :] = jnp.where(
            inside_col & (row < live), state_all[owner].astype(F32), 0.0
        ).astype(BF16)

    def multiply(owner, term, keep=False):
        block = jnp.dot(masked[...], gathered[owner, term], preferred_element_type=F32).astype(BF16)
        if keep:
            kept_terms[term, owner] = block
        acc[owner] += jnp.dot(comb[term], block, preferred_element_type=F32)

    def send_parts(owner):
        for index in range(4):
            slot = OFFSETS[index] + 2

            @pl.when(goes(index))
            def _():
                stage[index, owner] = acc[owner, slot * rows:(slot + 1) * rows, :].astype(BF16)
                part_copy(index, owner).start()

    def take_parts(owner):
        for index in range(4):
            @pl.when(comes(index))
            def _():
                part_copy(index, owner).wait_recv()
                acc[owner, home * rows:(home + 1) * rows, :] += landed[index, owner].astype(F32)

    def write_out(owner):
        for spot in range(4):
            @pl.when(owner == spot)
            def _():
                out_ref[:, spot * cols:(spot + 1) * cols] = acc[spot, home * rows:(home + 1) * rows, :]

    def end_slot(slot):
        @pl.loop(0, moved)
        def _(term):
            end_copy(slot, term, me).wait_recv()

            @pl.loop(0, 4)
            def _(owner):
                acc_end[slot, owner] += jnp.dot(
                    comb_end[slot, term], kept_terms[term, owner], preferred_element_type=F32
                )

    @pl.when(is_mid)
    def _():
        def first_pass(begin, end, keep):
            @pl.loop(begin, end)
            def _(term):
                arrived(other_mid, term)
                if not keep:
                    relay_copy(0, other_mid, term, near_end).start()
                arrived(near_end, term)
                relay_copy(1, near_end, term, other_mid).start()

                @pl.loop(0, 3)
                def _(which):
                    owner = jnp.where(which == 0, me, jnp.where(which == 1, other_mid, near_end))
                    multiply(owner, term, keep)

        first_pass(0, moved, True)
        first_pass(moved, terms, False)

        @pl.loop(0, 3)
        def _(which):
            send_parts(jnp.where(which == 0, me, jnp.where(which == 1, other_mid, near_end)))

        @pl.loop(0, moved)
        def _(term):
            arrived(far_end, term)
            multiply(far_end, term, True)

        @pl.loop(moved, terms)
        def _(term):
            arrived(far_end, term)
            relay_copy(2, far_end, term, near_end).start()
            multiply(far_end, term)

            for index in range(4):
                slot = OFFSETS[index] + 2

                @pl.when(term == turn_of(index, moved, terms))
                def _():
                    end_slot(slot)

                    @pl.when(goes(index))
                    def _():
                        stage_end[index] = acc_end[slot].astype(BF16)
                        part_end_copy(index).start()

        send_parts(far_end)
        end_slot(home)

        for index in range(4):
            @pl.when(comes(index))
            def _():
                part_end_copy(index).wait_recv()
                acc_end[home] += landed_end[index].astype(F32)

        back[...] = acc_end[home].astype(BF16)
        back_copy(near_end).start()

        @pl.loop(0, 4)
        def _(owner):
            take_parts(owner)
            write_out(owner)

    @pl.when(is_end)
    def _():
        turn = jnp.where(me == 0, 1, -1)

        @pl.loop(0, 4)
        def _(rank):
            owner = me + turn * rank

            @pl.loop(moved, terms)
            def _(term):
                @pl.when(rank > 0)
                def _():
                    arrived(owner, term)

                multiply(owner, term)

            send_parts(owner)

        @pl.loop(0, 4)
        def _(rank):
            take_parts(me + turn * rank)

        back_copy(me).wait_recv()
        acc[:, home * rows:(home + 1) * rows, :] += back_landed[...].astype(F32)

        @pl.loop(0, 4)
        def _(owner):
            write_out(owner)

    for index in range(4):
        @pl.when(goes(index))
        def _():
            @pl.loop(0, 4)
            def _(owner):
                part_copy(index, owner).wait_send()

            @pl.when(is_mid)
            def _():
                part_end_copy(index).wait_send()

    @pl.when(is_mid)
    def _():
        state_own(0, near_end).wait_send()
        state_own(1, other_mid).wait_send()
        state_relay(2, other_mid, near_end).wait_send()
        state_relay(3, near_end, other_mid).wait_send()
        state_relay(4, far_end, near_end).wait_send()

        @pl.loop(0, terms)
        def _(term):
            own_copy(0, term, other_mid).wait_send()
            relay_copy(1, near_end, term, other_mid).wait_send()

            @pl.when(term >= moved)
            def _():
                own_copy(1, term, near_end).wait_send()
                relay_copy(0, other_mid, term, near_end).wait_send()
                relay_copy(2, far_end, term, near_end).wait_send()

        back_copy(near_end).wait_send()

    @pl.when(is_end)
    def _():
        state_own(0, near_mid).wait_send()

        @pl.loop(0, terms)
        def _(term):
            own_copy(0, term, near_mid).wait_send()

        for slot in END_SLOTS:
            @pl.loop(0, moved)
            def _(term):
                end_copy(slot, term, near_mid).wait_send()


def turn_of(index, moved, terms):
    steps = terms - moved
    return moved + min(steps - 1, max(0, (steps * (4 * index - 2)) // 12))


def line_apply(sectors, slots, dims, channel_term, channel_out, coefs, state, right, left):
    terms, width, cols = right.shape
    rows = state.shape[0]
    channels = left.shape[0]
    cells = slots * terms
    moved = max(1, terms // 4)
    tall = slots * rows
    dma = pltpu.SemaphoreType.DMA
    any_space = pl.BlockSpec(memory_space=pl.ANY)
    return pl.pallas_call(
        functools.partial(line_kernel, sectors, moved),
        out_shape=pltpu.VMEM((rows, width), F32),
        in_specs=[any_space] * 7,
        out_specs=pl.BlockSpec(memory_space=pltpu.VMEM),
        scratch_shapes=[
            pltpu.SMEM(dims.shape, jnp.int32),
            pltpu.VMEM((channels,), jnp.int32),
            pltpu.VMEM((channels,), jnp.int32),
            pltpu.VMEM((channels,), BF16),
            pltpu.VMEM((8, 128), jnp.int32),
            pltpu.SMEM((8, 128), jnp.int32),
            pltpu.VMEM((channels, width), F32),
            pltpu.VMEM((channels, width), F32),
            pltpu.VMEM((cells, width), F32),
            pltpu.VMEM(left.shape, BF16),
            pltpu.VMEM((rows, width), F32),
            pltpu.VMEM(left.shape, BF16),
            pltpu.VMEM((4, rows, width), BF16),
            pltpu.VMEM((width, width), BF16),
            pltpu.VMEM((4, terms, width, cols), BF16),
            pltpu.VMEM((terms, tall, width), BF16),
            pltpu.VMEM((slots, moved, rows, width), BF16),
            pltpu.VMEM((moved, 4, width, cols), BF16),
            pltpu.VMEM((4, tall, cols), F32),
            pltpu.VMEM((slots, 4, rows, cols), F32),
            pltpu.VMEM((4, 4, rows, cols), BF16),
            pltpu.VMEM((4, 4, rows, cols), BF16),
            pltpu.VMEM((4, 4, rows, cols), BF16),
            pltpu.VMEM((4, 4, rows, cols), BF16),
            pltpu.VMEM((4, rows, cols), BF16),
            pltpu.VMEM((4, rows, cols), BF16),
            dma((8,)), dma((5,)), dma((4,)),
            dma((2, terms)), dma((3, terms)), dma((4, terms)),
            dma((slots, moved)), dma((slots, moved)),
            dma((4, 4)), dma((4, 4)), dma((4,)), dma((4,)), dma((2,)),
        ],
        compiler_params=pltpu.CompilerParams(
            has_side_effects=True, collective_id=0, vmem_limit_bytes=60 * 2**20
        ),
    )(dims, channel_term, channel_out, coefs, state, right, left)


def passed_along(value, axis, steps):
    count = lax.axis_size(axis)
    first, last = (max(0, -steps), min(count, count - steps))
    return lax.ppermute(value, axis, [(source, source + steps) for source in range(first, last)])


def gathered_apply(sector, live_dim, wave, right, combined, rows, slots):
    width = wave.shape[1]
    terms = right.shape[0]
    whole_state = lax.all_gather(wave, "pan", axis=0, tiled=True)
    indices = lax.iota(jnp.int32, width)
    inside = (indices[:, None] < live_dim) & (indices[None, :] < live_dim)
    masked = jnp.where(inside, whole_state, jnp.zeros((), BF16))
    right_full = lax.all_gather(right, "pan", axis=2, tiled=True)
    term_full = jnp.einsum("ik,wkq->wiq", masked, right_full, preferred_element_type=F32).astype(BF16)
    parts = jnp.einsum(
        "wjri,wiq->jrq", combined.reshape(terms, slots, rows, width), term_full,
        preferred_element_type=F32,
    )
    collected = parts[2]
    for offset in OFFSETS:
        collected = collected + passed_along(parts[offset + 2], "sec", offset)
    return collected


def on_device(
    wave_state, right_blocks, left_blocks, coupling, channel_term, channel_out, sector_dims
):
    rows, width = wave_state.shape[1:]
    terms = right_blocks.shape[1]
    slots = 5
    sector = lax.axis_index("sec")
    live_dim = sector_dims[0]
    if lax.axis_size("pan") == 4 and right_blocks.shape[3] % 128 == 0:
        collected = line_apply(
            lax.axis_size("sec"), slots, sector_dims, channel_term, channel_out, coupling,
            wave_state[0], right_blocks[0], left_blocks,
        )
    else:
        cells = channel_term * slots + channel_out - sector + 2
        coefs = coupling.astype(F32)
        combined = combine(cells, coefs, left_blocks, terms * slots)
        collected = gathered_apply(
            sector, live_dim, wave_state[0], right_blocks[0], combined, rows, slots
        )
    indices = lax.iota(jnp.int32, width)
    row_ids = lax.axis_index("pan") * rows + lax.iota(jnp.int32, rows)
    kept_mask = (row_ids[:, None] < live_dim) & (indices[None, :] < live_dim)
    return jnp.where(kept_mask, collected, jnp.zeros((), F32))[None]


def solution(mesh):
    return jax.shard_map(
        on_device,
        mesh=mesh,
        in_specs=(
            P("sec", "pan", None),
            P("sec", None, None, "pan"),
            P("sec", "pan", None),
            P("sec"),
            P("sec"),
            P("sec"),
            P("sec"),
        ),
        out_specs=P("sec", "pan", None),
        check_vma=False,
    )
```

```python
import functools

import jax
import jax.numpy as jnp
from jax import lax
from jax.experimental import pallas as pl
from jax.experimental.pallas import tpu as pltpu
from jax.sharding import PartitionSpec as P

OFFSETS = (-2, -1, 1, 2)
END_SLOTS = (0, 1, 3, 4, 2)
F32 = jnp.float32
BF16 = jnp.bfloat16


def combine_kernel(cell_ref, coef_ref, left_ref, out_ref, acc_ref):
    acc_ref[...] = jnp.zeros_like(acc_ref)

    @pl.loop(0, left_ref.shape[0])
    def _(channel):
        cell = cell_ref[channel]
        acc_ref[cell] += left_ref[channel].astype(F32) * coef_ref[channel]

    @pl.loop(0, out_ref.shape[0])
    def _(cell):
        out_ref[cell] = acc_ref[cell].astype(BF16)


def combine(cells, coefs, left_blocks, cell_count):
    channels, rows, width = left_blocks.shape
    step = min(rows, 32)
    return pl.pallas_call(
        combine_kernel,
        grid=(rows // step,),
        in_specs=[
            pl.BlockSpec(memory_space=pltpu.SMEM),
            pl.BlockSpec(memory_space=pltpu.SMEM),
            pl.BlockSpec((channels, step, width), lambda i: (0, i, 0)),
        ],
        out_specs=pl.BlockSpec((cell_count, step, width), lambda i: (0, i, 0)),
        out_shape=jax.ShapeDtypeStruct((cell_count, rows, width), BF16),
        scratch_shapes=[pltpu.VMEM((cell_count, step, width), F32)],
        compiler_params=pltpu.CompilerParams(vmem_limit_bytes=48 * 2**20),
    )(cells, coefs, left_blocks)


def read_channels(slots, terms, sector, term, out_id, coef, coefs, kept, filled, table):
    count = term.shape[0]
    cells = slots * terms
    width = coefs.shape[1]
    cell = (term[...] * slots + out_id[...] - sector + 2).astype(F32)
    cell_row = jnp.broadcast_to(cell[None, :], (count, count))
    coef_row = jnp.broadcast_to(coef[...].astype(F32)[None, :], (count, count))
    down = lax.broadcasted_iota(jnp.int32, (count, count), 0)
    across = lax.broadcasted_iota(jnp.int32, (count, count), 1)

    def total(mask, values, axis):
        return jnp.sum(jnp.where(mask, values, 0.0), axis=axis, keepdims=True)

    cell_col = total(down == across, cell_row, 1)
    same = cell_col == cell_row
    precedes = (cell_col < cell_row) | (same & (down < across))
    follows = (cell_row < cell_col) | (same & (across < down))
    rank_row = total(precedes, 1.0, 0)
    rank_col = total(follows, 1.0, 1)
    again = jnp.where(total(same & (down < across), 1.0, 0) > 0, 1.0, 0.0)
    spot = rank_row == down.astype(F32)
    coefs[...] = jnp.broadcast_to(total(spot, coef_row, 1), (count, width))
    kept[...] = jnp.broadcast_to(
        total(spot, jnp.broadcast_to(again, (count, count)), 1), (count, width)
    )
    order = total(rank_col == across.astype(F32), down.astype(F32), 0)
    cell_ids = lax.broadcasted_iota(jnp.int32, (count, cells), 1).astype(F32)
    last = total(jnp.broadcast_to(cell_col, (count, cells)) <= cell_ids, 1.0, 0) - 1.0
    ids_down = lax.broadcasted_iota(jnp.int32, (cells, count), 0).astype(F32)
    held = total(ids_down == jnp.broadcast_to(cell[None, :], (cells, count)), 1.0, 1)
    filled[...] = jnp.broadcast_to(jnp.where(held > 0, 1.0, 0.0), (cells, width))
    table[0:1, 0:count] = order.astype(jnp.int32)
    table[1:2, 0:cells] = jnp.maximum(last, 0.0).astype(jnp.int32)


def line_kernel(
    sectors, dims_ref, term_ref, out_id_ref, coef_ref, state_ref, right_ref, left_ref,
    out_ref,
    dims, term_ids, out_ids, coef, table, spots, coefs, kept, filled,
    left_all, running, summed,
    state_all, masked, gathered, blocks, comb, comb_end, acc, acc_end,
    stage, landed, stage_end, landed_end, back, back_landed,
    local_sems, state_send, state_recv, own_send, relay_send, right_recv,
    end_send, end_recv, part_send, part_recv, part_end_send, part_end_recv, back_sems,
):
    terms, width, cols = right_ref.shape
    rows = state_ref.shape[0]
    slots = comb.shape[1] // rows
    home = slots // 2
    me = lax.axis_index("pan")
    sector = lax.axis_index("sec")
    is_mid = (me == 1) | (me == 2)
    is_end = jnp.logical_not(is_mid)
    near_end = jnp.where(me <= 1, 0, 3)
    other_mid = jnp.where(me <= 1, 2, 1)
    far_end = 3 - near_end
    near_mid = jnp.where(me <= 1, 1, 2)
    per = comb_end.shape[2]
    groups = terms // per
    early = 1
    inner = width - rows
    near_rows = pl.ds(pl.multiple_of(jnp.where(near_end == 0, 0, rows), rows), inner)
    far_rows = pl.ds(pl.multiple_of(far_end * rows, rows), rows)

    def remote(src, dst, send, recv, where, axis="pan"):
        return pltpu.make_async_remote_copy(
            src_ref=src, dst_ref=dst, send_sem=send, recv_sem=recv,
            device_id={axis: where}, device_id_type=pl.DeviceIdType.MESH,
        )

    def state_own(way, where):
        return remote(state_ref, state_all.at[me], state_send.at[way], state_recv.at[me], where)

    def state_relay(way, owner, where):
        block = state_all.at[owner]
        return remote(block, block, state_send.at[way], state_recv.at[owner], where)

    def state_wait(owner):
        state_relay(0, owner, me).wait_recv()

    def own_copy(way, term, where):
        return remote(
            right_ref.at[term], gathered.at[me, term],
            own_send.at[way, term], right_recv.at[me, term], where,
        )

    def relay_copy(way, owner, term, where):
        block = gathered.at[owner, term]
        return remote(block, block, relay_send.at[way, term], right_recv.at[owner, term], where)

    def block_copy(sems, way, owner, term, where):
        block = blocks.at[owner, term, near_rows]
        return remote(block, block, sems.at[way, term], right_recv.at[owner, term], where)

    def block_arrived(owner, term):
        block_copy(relay_send, 0, owner, term, me).wait_recv()

    def end_copy(slot, group, where):
        spot = pl.ds(pl.multiple_of(slot * rows, rows), rows)
        return remote(
            comb.at[pl.ds(group * per, per), spot, far_rows], comb_end.at[slot, group],
            end_send.at[slot, group], end_recv.at[slot, group], where,
        )

    def arrived(owner, term):
        block = gathered.at[owner, term]
        remote(block, block, relay_send.at[0, term], right_recv.at[owner, term], me).wait_recv()

    def part_copy(index, owner):
        return remote(
            stage.at[index, owner], landed.at[index, owner],
            part_send.at[index, owner], part_recv.at[index, owner], sector + OFFSETS[index], "sec",
        )

    def part_end_copy(index, owner):
        return remote(
            stage_end.at[index, owner], landed_end.at[index, owner],
            part_end_send.at[index, owner], part_end_recv.at[index, owner],
            sector + OFFSETS[index], "sec",
        )

    def back_copy(where):
        return remote(back, back_landed, back_sems.at[0], back_sems.at[1], where)

    def goes(index):
        target = sector + OFFSETS[index]
        return (target >= 0) & (target < sectors)

    def comes(index):
        source = sector - OFFSETS[index]
        return (source >= 0) & (source < sectors)

    barrier = pltpu.get_barrier_semaphore()

    def greet(axis, where):
        pl.semaphore_signal(
            barrier, inc=1, device_id={axis: where}, device_id_type=pl.DeviceIdType.MESH
        )

    greet("pan", jnp.where(is_mid, near_end, near_mid))

    @pl.when(is_mid)
    def _():
        greet("pan", other_mid)

    peers = jnp.where(is_mid, 2, 1)
    for index in range(4):
        peers = peers + goes(index).astype(jnp.int32)

        @pl.when(goes(index))
        def _():
            greet("sec", sector + OFFSETS[index])

    pl.semaphore_wait(barrier, peers)

    @pl.when(is_mid)
    def _():
        state_own(0, near_end).start()
        state_own(1, other_mid).start()

        @pl.loop(0, early)
        def _(term):
            own_copy(1, term, near_end).start()

        @pl.loop(0, 2 * early)
        def _(term):
            own_copy(0, term, other_mid).start()

    @pl.when(is_end)
    def _():
        state_own(0, near_mid).start()

        @pl.loop(0, terms)
        def _(term):
            own_copy(0, term, near_mid).start()

    small = [
        pltpu.make_async_copy(dims_ref, dims, local_sems.at[0]),
        pltpu.make_async_copy(term_ref, term_ids, local_sems.at[1]),
        pltpu.make_async_copy(out_id_ref, out_ids, local_sems.at[2]),
        pltpu.make_async_copy(coef_ref, coef, local_sems.at[3]),
    ]
    large = [
        pltpu.make_async_copy(left_ref, left_all, local_sems.at[4]),
        pltpu.make_async_copy(state_ref, state_all.at[me], local_sems.at[5]),
        pltpu.make_async_copy(right_ref, gathered.at[me], local_sems.at[6]),
    ]
    for copy in small + large:
        copy.start()
    for copy in small:
        copy.wait()
    read_channels(slots, terms, sector, term_ids, out_ids, coef, coefs, kept, filled, table)
    spots_copy = pltpu.make_async_copy(table, spots, local_sems.at[7])
    spots_copy.start()
    acc[...] = jnp.zeros_like(acc)
    acc_end[...] = jnp.zeros_like(acc_end)
    running[...] = jnp.zeros_like(running)

    live = dims[0]
    inside_col = lax.broadcasted_iota(jnp.int32, (rows, width), 1) < live

    def mask_rows(owner):
        row = lax.broadcasted_iota(jnp.int32, (rows, width), 0) + owner * rows
        spot = pl.ds(pl.multiple_of(owner * rows, rows), rows)
        masked[spot, :] = jnp.where(
            inside_col & (row < live), state_all[owner].astype(F32), 0.0
        ).astype(BF16)

    def block_of(owner, term, spot):
        return jnp.dot(
            masked[spot, :], gathered[owner, term], preferred_element_type=F32
        ).astype(BF16)

    large[1].wait()
    large[2].wait()

    @pl.when(is_mid)
    def _():
        state_wait(other_mid)
        state_relay(2, other_mid, near_end).start()
        state_wait(near_end)
        state_relay(3, near_end, other_mid).start()

        @pl.loop(2 * early, terms)
        def _(term):
            own_copy(0, term, other_mid).start()

        @pl.loop(0, 3)
        def _(which):
            mask_rows(jnp.where(which == 0, me, jnp.where(which == 1, other_mid, near_end)))

        @pl.loop(early, terms)
        def _(term):
            blocks[me, term, near_rows, :] = block_of(me, term, near_rows)
            block_copy(own_send, 1, me, term, near_end).start()

    spots_copy.wait()
    large[0].wait()
    channels = left_all.shape[0]

    def inside(spot):
        return jnp.minimum(jnp.maximum(spot, 0), channels - 1)

    @pl.loop(0, channels)
    def _(step):
        row = pl.ds(step, 1)
        total = running[...] * kept[row, :] + left_all[inside(spots[0, step])].astype(F32) * coefs[row, :]
        running[...] = total
        summed[step] = total.astype(BF16)

    @pl.loop(0, terms)
    def _(term):
        for slot in range(slots):
            cell = term * slots + slot
            value = summed[inside(spots[1, cell])].astype(F32) * filled[pl.ds(cell, 1), :]
            comb[term, slot * rows:(slot + 1) * rows, :] = value.astype(BF16)

    @pl.when(is_end)
    def _():
        for slot in END_SLOTS:
            @pl.loop(0, groups)
            def _(group):
                end_copy(slot, group, near_mid).start()

    def send_parts(owner):
        for index in range(4):
            slot = OFFSETS[index] + 2

            @pl.when(goes(index))
            def _():
                stage[index, owner] = acc[owner, slot * rows:(slot + 1) * rows, :].astype(BF16)
                part_copy(index, owner).start()

    def take_parts(owner):
        for index in range(4):
            @pl.when(comes(index))
            def _():
                part_copy(index, owner).wait_recv()
                acc[owner, home * rows:(home + 1) * rows, :] += landed[index, owner].astype(F32)

    def write_out(owner):
        for spot in range(4):
            @pl.when(owner == spot)
            def _():
                out_ref[:, spot * cols:(spot + 1) * cols] = acc[spot, home * rows:(home + 1) * rows, :]

    def end_multiply(slot, group, owner):
        left = [comb_end[slot, group, spot] for spot in range(per)]
        right = [blocks[owner, group * per + spot, far_rows, :] for spot in range(per)]
        acc_end[slot, owner] += jnp.dot(
            jnp.concatenate(left, axis=1), jnp.concatenate(right, axis=0),
            preferred_element_type=F32,
        )

    def send_end_parts(index, owner):
        @pl.when(goes(index))
        def _():
            stage_end[index, owner] = acc_end[OFFSETS[index] + 2, owner].astype(BF16)
            part_end_copy(index, owner).start()

    @pl.when(is_mid)
    def _():
        def near_owner(which):
            return jnp.where(which == 0, me, jnp.where(which == 1, other_mid, near_end))

        def multiply(owner, term):
            acc[owner] += jnp.dot(comb[term], blocks[owner, term], preferred_element_type=F32)

        state_wait(far_end)
        mask_rows(far_end)

        @pl.loop(0, early)
        def _(term):
            blocks[me, term, near_rows, :] = block_of(me, term, near_rows)

        @pl.loop(0, terms)
        def _(term):
            blocks[me, term, far_rows, :] = block_of(me, term, far_rows)

        everything = slice(None)

        @pl.loop(0, terms)
        def _(term):
            arrived(other_mid, term)
            blocks[other_mid, term] = block_of(other_mid, term, everything)
            block_copy(relay_send, 0, other_mid, term, near_end).start()
            arrived(near_end, term)
            relay_copy(1, near_end, term, other_mid).start()
            blocks[near_end, term] = block_of(near_end, term, everything)

            @pl.loop(0, 3)
            def _(which):
                multiply(near_owner(which), term)

        @pl.loop(0, 3)
        def _(which):
            send_parts(near_owner(which))

        @pl.loop(0, terms)
        def _(term):
            arrived(far_end, term)
            blocks[far_end, term] = block_of(far_end, term, everything)
            block_copy(relay_send, 2, far_end, term, near_end).start()
            multiply(far_end, term)

            for index in range(4):
                slot = OFFSETS[index] + 2

                @pl.when(term == (index + 1) * terms // 4 - 1)
                def _():
                    @pl.loop(0, groups)
                    def _(group):
                        end_copy(slot, group, me).wait_recv()

                        @pl.loop(0, 3)
                        def _(which):
                            end_multiply(slot, group, near_owner(which))

                    @pl.loop(0, 3)
                    def _(which):
                        send_end_parts(index, near_owner(which))

        send_parts(far_end)

        for index in range(4):
            @pl.loop(0, groups)
            def _(group):
                end_multiply(OFFSETS[index] + 2, group, far_end)

            send_end_parts(index, far_end)

        @pl.loop(0, groups)
        def _(group):
            end_copy(home, group, me).wait_recv()

            @pl.loop(0, 4)
            def _(owner):
                end_multiply(home, group, owner)

        for index in range(4):
            @pl.when(comes(index))
            def _():
                @pl.loop(0, 4)
                def _(owner):
                    part_end_copy(index, owner).wait_recv()
                    acc_end[home, owner] += landed_end[index, owner].astype(F32)

        back[...] = acc_end[home].astype(BF16)
        back_copy(near_end).start()

        @pl.loop(0, 4)
        def _(owner):
            take_parts(owner)
            write_out(owner)

    @pl.when(is_end)
    def _():
        turn = jnp.where(me == 0, 1, -1)
        state_wait(near_mid)
        state_wait(3 - near_mid)

        @pl.loop(0, 3)
        def _(rank):
            mask_rows(me + turn * rank)

        def multiply(owner, term, block):
            acc[owner] += jnp.dot(comb[term, :, near_rows], block, preferred_element_type=F32)

        @pl.loop(0, terms)
        def _(term):
            multiply(me, term, block_of(me, term, near_rows))

        send_parts(me)

        @pl.loop(0, early)
        def _(term):
            arrived(near_mid, term)
            multiply(near_mid, term, block_of(near_mid, term, near_rows))

        @pl.loop(1, 4)
        def _(rank):
            owner = me + turn * rank

            @pl.loop(jnp.where(rank == 1, early, 0), terms)
            def _(term):
                block_arrived(owner, term)
                multiply(owner, term, blocks[owner, term, near_rows, :])

            send_parts(owner)

        @pl.loop(0, 4)
        def _(rank):
            take_parts(me + turn * rank)

        back_copy(me).wait_recv()
        acc[:, home * rows:(home + 1) * rows, :] += back_landed[...].astype(F32)

        @pl.loop(0, 4)
        def _(owner):
            write_out(owner)

    for index in range(4):
        @pl.when(goes(index))
        def _():
            @pl.loop(0, 4)
            def _(owner):
                part_copy(index, owner).wait_send()

                @pl.when(is_mid)
                def _():
                    part_end_copy(index, owner).wait_send()

    @pl.when(is_mid)
    def _():
        state_own(0, near_end).wait_send()
        state_own(1, other_mid).wait_send()
        state_relay(2, other_mid, near_end).wait_send()
        state_relay(3, near_end, other_mid).wait_send()

        @pl.loop(0, early)
        def _(term):
            own_copy(1, term, near_end).wait_send()

        @pl.loop(early, terms)
        def _(term):
            block_copy(own_send, 1, me, term, near_end).wait_send()

        @pl.loop(0, terms)
        def _(term):
            own_copy(0, term, other_mid).wait_send()
            relay_copy(1, near_end, term, other_mid).wait_send()
            block_copy(relay_send, 0, other_mid, term, near_end).wait_send()
            block_copy(relay_send, 2, far_end, term, near_end).wait_send()

        back_copy(near_end).wait_send()

    @pl.when(is_end)
    def _():
        state_own(0, near_mid).wait_send()

        @pl.loop(0, terms)
        def _(term):
            own_copy(0, term, near_mid).wait_send()

        for slot in END_SLOTS:
            @pl.loop(0, groups)
            def _(group):
                end_copy(slot, group, near_mid).wait_send()


def line_apply(sectors, slots, dims, channel_term, channel_out, coefs, state, right, left):
    terms, width, cols = right.shape
    rows = state.shape[0]
    channels = left.shape[0]
    cells = slots * terms
    per = 4
    groups = terms // per
    tall = slots * rows
    dma = pltpu.SemaphoreType.DMA
    any_space = pl.BlockSpec(memory_space=pl.ANY)
    return pl.pallas_call(
        functools.partial(line_kernel, sectors),
        out_shape=pltpu.VMEM((rows, width), F32),
        in_specs=[any_space] * 7,
        out_specs=pl.BlockSpec(memory_space=pltpu.VMEM),
        scratch_shapes=[
            pltpu.SMEM(dims.shape, jnp.int32),
            pltpu.VMEM((channels,), jnp.int32),
            pltpu.VMEM((channels,), jnp.int32),
            pltpu.VMEM((channels,), BF16),
            pltpu.VMEM((8, 128), jnp.int32),
            pltpu.SMEM((8, 128), jnp.int32),
            pltpu.VMEM((channels, width), F32),
            pltpu.VMEM((channels, width), F32),
            pltpu.VMEM((cells, width), F32),
            pltpu.VMEM(left.shape, BF16),
            pltpu.VMEM((rows, width), F32),
            pltpu.VMEM(left.shape, BF16),
            pltpu.VMEM((4, rows, width), BF16),
            pltpu.VMEM((width, width), BF16),
            pltpu.VMEM((4, terms, width, cols), BF16),
            pltpu.VMEM((4, terms, width, cols), BF16),
            pltpu.VMEM((terms, tall, width), BF16),
            pltpu.VMEM((slots, groups, per, rows, rows), BF16),
            pltpu.VMEM((4, tall, cols), F32),
            pltpu.VMEM((slots, 4, rows, cols), F32),
            pltpu.VMEM((4, 4, rows, cols), BF16),
            pltpu.VMEM((4, 4, rows, cols), BF16),
            pltpu.VMEM((4, 4, rows, cols), BF16),
            pltpu.VMEM((4, 4, rows, cols), BF16),
            pltpu.VMEM((4, rows, cols), BF16),
            pltpu.VMEM((4, rows, cols), BF16),
            dma((8,)), dma((4,)), dma((4,)),
            dma((2, terms)), dma((3, terms)), dma((4, terms)),
            dma((slots, groups)), dma((slots, groups)),
            dma((4, 4)), dma((4, 4)), dma((4, 4)), dma((4, 4)), dma((2,)),
        ],
        compiler_params=pltpu.CompilerParams(
            has_side_effects=True, collective_id=0, vmem_limit_bytes=60 * 2**20
        ),
    )(dims, channel_term, channel_out, coefs, state, right, left)


def passed_along(value, axis, steps):
    count = lax.axis_size(axis)
    first, last = (max(0, -steps), min(count, count - steps))
    return lax.ppermute(value, axis, [(source, source + steps) for source in range(first, last)])


def gathered_apply(sector, live_dim, wave, right, combined, rows, slots):
    width = wave.shape[1]
    terms = right.shape[0]
    whole_state = lax.all_gather(wave, "pan", axis=0, tiled=True)
    indices = lax.iota(jnp.int32, width)
    inside = (indices[:, None] < live_dim) & (indices[None, :] < live_dim)
    masked = jnp.where(inside, whole_state, jnp.zeros((), BF16))
    right_full = lax.all_gather(right, "pan", axis=2, tiled=True)
    term_full = jnp.einsum("ik,wkq->wiq", masked, right_full, preferred_element_type=F32).astype(BF16)
    parts = jnp.einsum(
        "wjri,wiq->jrq", combined.reshape(terms, slots, rows, width), term_full,
        preferred_element_type=F32,
    )
    collected = parts[2]
    for offset in OFFSETS:
        collected = collected + passed_along(parts[offset + 2], "sec", offset)
    return collected


def on_device(
    wave_state, right_blocks, left_blocks, coupling, channel_term, channel_out, sector_dims
):
    rows, width = wave_state.shape[1:]
    terms = right_blocks.shape[1]
    slots = 5
    sector = lax.axis_index("sec")
    live_dim = sector_dims[0]
    if lax.axis_size("pan") == 4 and right_blocks.shape[3] % 128 == 0 and terms % 4 == 0:
        collected = line_apply(
            lax.axis_size("sec"), slots, sector_dims, channel_term, channel_out, coupling,
            wave_state[0], right_blocks[0], left_blocks,
        )
    else:
        cells = channel_term * slots + channel_out - sector + 2
        coefs = coupling.astype(F32)
        combined = combine(cells, coefs, left_blocks, terms * slots)
        collected = gathered_apply(
            sector, live_dim, wave_state[0], right_blocks[0], combined, rows, slots
        )
    indices = lax.iota(jnp.int32, width)
    row_ids = lax.axis_index("pan") * rows + lax.iota(jnp.int32, rows)
    kept_mask = (row_ids[:, None] < live_dim) & (indices[None, :] < live_dim)
    return jnp.where(kept_mask, collected, jnp.zeros((), F32))[None]


def solution(mesh):
    return jax.shard_map(
        on_device,
        mesh=mesh,
        in_specs=(
            P("sec", "pan", None),
            P("sec", None, None, "pan"),
            P("sec", "pan", None),
            P("sec"),
            P("sec"),
            P("sec"),
            P("sec"),
        ),
        out_specs=P("sec", "pan", None),
        check_vma=False,
    )
```

```python
import functools

import jax
import jax.numpy as jnp
from jax import lax
from jax.experimental import pallas as pl
from jax.experimental.pallas import tpu as pltpu
from jax.sharding import PartitionSpec as P

OFFSETS = (-2, -1, 1, 2)
END_SLOTS = (0, 1, 3, 4)
F32 = jnp.float32
BF16 = jnp.bfloat16


def combine_kernel(cell_ref, coef_ref, left_ref, out_ref, acc_ref):
    acc_ref[...] = jnp.zeros_like(acc_ref)

    @pl.loop(0, left_ref.shape[0])
    def _(channel):
        cell = cell_ref[channel]
        acc_ref[cell] += left_ref[channel].astype(F32) * coef_ref[channel]

    @pl.loop(0, out_ref.shape[0])
    def _(cell):
        out_ref[cell] = acc_ref[cell].astype(BF16)


def combine(cells, coefs, left_blocks, cell_count):
    channels, rows, width = left_blocks.shape
    step = min(rows, 32)
    return pl.pallas_call(
        combine_kernel,
        grid=(rows // step,),
        in_specs=[
            pl.BlockSpec(memory_space=pltpu.SMEM),
            pl.BlockSpec(memory_space=pltpu.SMEM),
            pl.BlockSpec((channels, step, width), lambda i: (0, i, 0)),
        ],
        out_specs=pl.BlockSpec((cell_count, step, width), lambda i: (0, i, 0)),
        out_shape=jax.ShapeDtypeStruct((cell_count, rows, width), BF16),
        scratch_shapes=[pltpu.VMEM((cell_count, step, width), F32)],
        compiler_params=pltpu.CompilerParams(vmem_limit_bytes=48 * 2**20),
    )(cells, coefs, left_blocks)


def read_channels(slots, terms, sector, term, out_id, coef, coefs, kept, filled, table):
    count = term.shape[0]
    cells = slots * terms
    width = coefs.shape[1]
    cell = (term[...] * slots + out_id[...] - sector + 2).astype(F32)
    cell_row = jnp.broadcast_to(cell[None, :], (count, count))
    coef_row = jnp.broadcast_to(coef[...].astype(F32)[None, :], (count, count))
    down = lax.broadcasted_iota(jnp.int32, (count, count), 0)
    across = lax.broadcasted_iota(jnp.int32, (count, count), 1)

    def total(mask, values, axis):
        return jnp.sum(jnp.where(mask, values, 0.0), axis=axis, keepdims=True)

    cell_col = total(down == across, cell_row, 1)
    same = cell_col == cell_row
    precedes = (cell_col < cell_row) | (same & (down < across))
    follows = (cell_row < cell_col) | (same & (across < down))
    rank_row = total(precedes, 1.0, 0)
    rank_col = total(follows, 1.0, 1)
    again = jnp.where(total(same & (down < across), 1.0, 0) > 0, 1.0, 0.0)
    spot = rank_row == down.astype(F32)
    coefs[...] = jnp.broadcast_to(total(spot, coef_row, 1), (count, width))
    kept[...] = jnp.broadcast_to(
        total(spot, jnp.broadcast_to(again, (count, count)), 1), (count, width)
    )
    order = total(rank_col == across.astype(F32), down.astype(F32), 0)
    cell_ids = lax.broadcasted_iota(jnp.int32, (count, cells), 1).astype(F32)
    last = total(jnp.broadcast_to(cell_col, (count, cells)) <= cell_ids, 1.0, 0) - 1.0
    ids_down = lax.broadcasted_iota(jnp.int32, (cells, count), 0).astype(F32)
    held = total(ids_down == jnp.broadcast_to(cell[None, :], (cells, count)), 1.0, 1)
    filled[...] = jnp.broadcast_to(jnp.where(held > 0, 1.0, 0.0), (cells, width))
    table[0:1, 0:count] = order.astype(jnp.int32)
    table[1:2, 0:cells] = jnp.maximum(last, 0.0).astype(jnp.int32)


def line_kernel(
    sectors, detours, least, dims_ref, term_ref, out_id_ref, coef_ref, state_ref, right_ref, left_ref,
    out_ref,
    dims, term_ids, out_ids, coef, table, spots, coefs, kept, filled,
    left_all, running, summed,
    state_all, masked, gathered, blocks, comb, comb_end, comb_extra, passing, acc, acc_end,
    stage, landed, stage_end, landed_end, back, back_landed,
    local_sems, state_send, state_recv, own_send, relay_send, right_recv,
    end_send, end_recv, extra_send, extra_recv, home_send, home_recv,
    passing_send, passing_recv, part_send, part_recv, part_end_send, part_end_recv, back_sems,
):
    terms, width, cols = right_ref.shape
    rows = state_ref.shape[0]
    slots = comb.shape[1] // rows
    home = slots // 2
    me = lax.axis_index("pan")
    sector = lax.axis_index("sec")
    is_mid = (me == 1) | (me == 2)
    is_end = jnp.logical_not(is_mid)
    near_end = jnp.where(me <= 1, 0, 3)
    other_mid = jnp.where(me <= 1, 2, 1)
    far_end = 3 - near_end
    near_mid = jnp.where(me <= 1, 1, 2)
    per = comb_end.shape[2]
    groups = terms // per
    edge = (sector < 2) | (sector >= sectors - 2)
    cut = terms - jnp.where(edge, comb_extra.shape[1], least)
    turned = terms - detours
    low = sector < sectors // 2
    outer = jnp.where(low, sector - 2, sector + 2)
    served = jnp.where(low, sector + 2, sector - 2)
    strips = home_send.shape[0]
    strip = rows // strips
    half = rows // 2
    inner = width - rows
    near_rows = pl.ds(pl.multiple_of(jnp.where(near_end == 0, 0, rows), rows), inner)
    far_rows = pl.ds(pl.multiple_of(far_end * rows, rows), rows)
    short_rows = pl.ds(pl.multiple_of(jnp.where(near_end == 0, 0, 2 * rows), rows), inner - rows)
    extra_rows = pl.ds(pl.multiple_of(other_mid * rows, rows), rows)

    def remote(src, dst, send, recv, where, axis="pan"):
        return pltpu.make_async_remote_copy(
            src_ref=src, dst_ref=dst, send_sem=send, recv_sem=recv,
            device_id={axis: where}, device_id_type=pl.DeviceIdType.MESH,
        )

    def state_copy(way, owner, part, where):
        block = state_all.at[owner, pl.ds(part * half, half)]
        return remote(
            block, block, state_send.at[way, part], state_recv.at[owner, part], where
        )

    def state_wait(owner):
        for part in range(2):
            state_copy(0, owner, part, me).wait_recv()

    def own_copy(term, where):
        return remote(
            right_ref.at[term], gathered.at[me, term],
            own_send.at[0, term], right_recv.at[me, term], where,
        )

    def relay_copy(owner, term, where):
        block = gathered.at[owner, term]
        return remote(block, block, relay_send.at[1, term], right_recv.at[owner, term], where)

    def block_copy(sems, way, owner, term, where, spot):
        block = blocks.at[owner, term, spot]
        return remote(block, block, sems.at[way, term], right_recv.at[owner, term], where)

    def send_block(sems, way, owner, term):
        @pl.when(term < cut)
        def _():
            block_copy(sems, way, owner, term, near_end, near_rows).start()

        @pl.when(term >= cut)
        def _():
            block_copy(sems, way, owner, term, near_end, short_rows).start()

    def sent_block(sems, way, owner, term):
        @pl.when(term < cut)
        def _():
            block_copy(sems, way, owner, term, near_end, near_rows).wait_send()

        @pl.when(term >= cut)
        def _():
            block_copy(sems, way, owner, term, near_end, short_rows).wait_send()

    def turn_off(term):
        index = term - turned
        return remote(
            blocks.at[me, term, near_rows], passing.at[index],
            passing_send.at[0, index], passing_recv.at[index], outer, "sec",
        )

    def pass_on(term):
        index = term - turned
        return pltpu.make_async_remote_copy(
            src_ref=passing.at[index], dst_ref=blocks.at[me, term, near_rows],
            send_sem=passing_send.at[1, index], recv_sem=right_recv.at[me, term],
            device_id={"sec": served, "pan": near_end}, device_id_type=pl.DeviceIdType.MESH,
        )

    def block_arrived(owner, term, spot):
        block_copy(relay_send, 0, owner, term, me, spot).wait_recv()

    def end_copy(slot, group, where):
        spot = pl.ds(pl.multiple_of(slot * rows, rows), rows)
        return remote(
            comb.at[pl.ds(group * per, per), spot, far_rows], comb_end.at[slot, group],
            end_send.at[slot, group], end_recv.at[slot, group], where,
        )

    def extra_copy(slot, term, where):
        spot = pl.ds(pl.multiple_of(slot * rows, rows), rows)
        index = terms - 1 - term
        return remote(
            comb.at[term, spot, extra_rows], comb_extra.at[slot, index],
            extra_send.at[slot, index], extra_recv.at[slot, index], where,
        )

    def home_copy(part, group, where):
        source = pl.ds(home * rows + part * strip, strip)
        spot = pl.ds(part * strip, strip)
        return remote(
            comb.at[pl.ds(group * per, per), source, far_rows], comb_end.at[home, group, :, spot],
            home_send.at[part, group], home_recv.at[part, group], where,
        )

    def arrived(owner, term):
        block = gathered.at[owner, term]
        remote(block, block, relay_send.at[0, term], right_recv.at[owner, term], me).wait_recv()

    def part_copy(index, owner):
        return remote(
            stage.at[index, owner], landed.at[index, owner],
            part_send.at[index, owner], part_recv.at[index, owner], sector + OFFSETS[index], "sec",
        )

    def part_end_copy(index, owner):
        return remote(
            stage_end.at[index, owner], landed_end.at[index, owner],
            part_end_send.at[index, owner], part_end_recv.at[index, owner],
            sector + OFFSETS[index], "sec",
        )

    def back_copy(part, where):
        spot = pl.ds(part * strip, strip)
        return remote(
            back.at[:, spot], back_landed.at[:, spot],
            back_sems.at[0, part], back_sems.at[1, part], where,
        )

    def goes(index):
        target = sector + OFFSETS[index]
        return (target >= 0) & (target < sectors)

    def comes(index):
        source = sector - OFFSETS[index]
        return (source >= 0) & (source < sectors)

    small = [
        pltpu.make_async_copy(dims_ref, dims, local_sems.at[0]),
        pltpu.make_async_copy(term_ref, term_ids, local_sems.at[1]),
        pltpu.make_async_copy(out_id_ref, out_ids, local_sems.at[2]),
        pltpu.make_async_copy(coef_ref, coef, local_sems.at[3]),
    ]
    large = [
        pltpu.make_async_copy(left_ref, left_all, local_sems.at[4]),
        pltpu.make_async_copy(state_ref, state_all.at[me], local_sems.at[5]),
        pltpu.make_async_copy(right_ref, gathered.at[me], local_sems.at[6]),
    ]
    for copy in large[1:2] + small + large[2:] + large[:1]:
        copy.start()

    barrier = pltpu.get_barrier_semaphore()

    def greet(axis, where):
        pl.semaphore_signal(
            barrier, inc=1, device_id={axis: where}, device_id_type=pl.DeviceIdType.MESH
        )

    greet("pan", jnp.where(is_mid, near_end, near_mid))

    @pl.when(is_mid)
    def _():
        greet("pan", other_mid)

    peers = jnp.where(is_mid, 2, 1)
    for index in range(4):
        peers = peers + goes(index).astype(jnp.int32)

        @pl.when(goes(index))
        def _():
            greet("sec", sector + OFFSETS[index])

    pl.semaphore_wait(barrier, peers)

    large[1].wait()

    @pl.when(is_mid)
    def _():
        for part in range(2):
            state_copy(0, me, part, near_end).start()
            state_copy(1, me, part, other_mid).start()

        @pl.loop(0, 2)
        def _(term):
            own_copy(term, other_mid).start()

    @pl.when(is_end)
    def _():
        for part in range(2):
            state_copy(0, me, part, near_mid).start()

        @pl.loop(0, terms)
        def _(term):
            own_copy(term, near_mid).start()

    for copy in small:
        copy.wait()
    read_channels(slots, terms, sector, term_ids, out_ids, coef, coefs, kept, filled, table)
    spots_copy = pltpu.make_async_copy(table, spots, local_sems.at[7])
    spots_copy.start()
    acc[...] = jnp.zeros_like(acc)
    acc_end[...] = jnp.zeros_like(acc_end)
    running[...] = jnp.zeros_like(running)

    live = dims[0]
    inside_col = lax.broadcasted_iota(jnp.int32, (rows, width), 1) < live

    def mask_rows(owner):
        row = lax.broadcasted_iota(jnp.int32, (rows, width), 0) + owner * rows
        spot = pl.ds(pl.multiple_of(owner * rows, rows), rows)
        masked[spot, :] = jnp.where(
            inside_col & (row < live), state_all[owner].astype(F32), 0.0
        ).astype(BF16)

    def block_of(owner, term, spot):
        return jnp.dot(
            masked[spot, :], gathered[owner, term], preferred_element_type=F32
        ).astype(BF16)

    large[2].wait()

    @pl.when(is_mid)
    def _():
        for part in range(2):
            state_copy(0, other_mid, part, me).wait_recv()
            state_copy(2, other_mid, part, near_end).start()
            state_copy(0, near_end, part, me).wait_recv()
            state_copy(3, near_end, part, other_mid).start()

        @pl.loop(2, terms)
        def _(term):
            own_copy(term, other_mid).start()

        @pl.loop(0, 3)
        def _(which):
            mask_rows(jnp.where(which == 0, me, jnp.where(which == 1, other_mid, near_end)))

        @pl.loop(0, terms)
        def _(term):
            blocks[me, term, near_rows, :] = block_of(me, term, near_rows)
            turns = jnp.logical_not(edge) & (term >= turned)

            @pl.when(turns)
            def _():
                turn_off(term).start()

            @pl.when(jnp.logical_not(turns))
            def _():
                send_block(own_send, 1, me, term)

    spots_copy.wait()
    large[0].wait()
    channels = left_all.shape[0]

    def inside(spot):
        return jnp.minimum(jnp.maximum(spot, 0), channels - 1)

    @pl.loop(0, channels)
    def _(step):
        row = pl.ds(step, 1)
        total = running[...] * kept[row, :] + left_all[inside(spots[0, step])].astype(F32) * coefs[row, :]
        running[...] = total
        summed[step] = total.astype(BF16)

    @pl.loop(0, terms)
    def _(term):
        for slot in range(slots):
            cell = term * slots + slot
            value = summed[inside(spots[1, cell])].astype(F32) * filled[pl.ds(cell, 1), :]
            comb[term, slot * rows:(slot + 1) * rows, :] = value.astype(BF16)

    @pl.when(is_end)
    def _():
        for index, slot in enumerate(END_SLOTS):
            @pl.when(goes(index))
            def _():
                @pl.loop(cut, terms)
                def _(term):
                    extra_copy(slot, term, near_mid).start()

                @pl.loop(0, groups)
                def _(group):
                    end_copy(slot, group, near_mid).start()

        @pl.loop(cut, terms)
        def _(term):
            extra_copy(home, term, near_mid).start()

        @pl.loop(0, strips)
        def _(part):
            @pl.loop(0, groups)
            def _(group):
                home_copy(part, group, near_mid).start()

    def across(index):
        return (sector // 2 + (sector + OFFSETS[index]) // 2) % 4 == 3

    def send_parts(owner):
        for index, slot in enumerate(END_SLOTS):
            stage[index, owner] = acc[owner, slot * rows:(slot + 1) * rows, :].astype(BF16)

        for first in (True, False):
            for index in range(4):
                @pl.when(goes(index) & (across(index) == first))
                def _():
                    part_copy(index, owner).start()

    def take_parts(owner):
        for index in range(4):
            @pl.when(comes(index))
            def _():
                part_copy(index, owner).wait_recv()
                acc[owner, home * rows:(home + 1) * rows, :] += landed[index, owner].astype(F32)

    def write_out(owner):
        for spot in range(4):
            @pl.when(owner == spot)
            def _():
                out_ref[:, spot * cols:(spot + 1) * cols] = acc[spot, home * rows:(home + 1) * rows, :]

    def far_blocks(owner, group):
        return jnp.concatenate(
            [blocks[owner, group * per + index, far_rows, :] for index in range(per)], axis=0
        )

    def end_rows(slot, group, spot):
        return jnp.concatenate(
            [comb_end[slot, group, index, spot, :] for index in range(per)], axis=1
        )

    def add_end(slot, owners, spot, left, rights):
        for first in range(0, len(owners), 2):
            pair = owners[first:first + 2]
            product = jnp.dot(
                left, jnp.concatenate(rights[first:first + 2], axis=1), preferred_element_type=F32
            )
            for index, owner in enumerate(pair):
                acc_end[slot, owner, spot, :] += product[:, index * cols:(index + 1) * cols]

    def end_multiply(slot, group, owners, spot=slice(None)):
        rights = [far_blocks(owner, group) for owner in owners]
        add_end(slot, owners, spot, end_rows(slot, group, spot), rights)

    def extra_multiply(slot, owners, term):
        rights = [blocks[owner, term, extra_rows, :] for owner in owners]
        add_end(slot, owners, slice(None), comb_extra[slot, terms - 1 - term], rights)

    def add_far(left, right):
        product = jnp.dot(
            jnp.concatenate(left, axis=0), right, preferred_element_type=F32
        )
        for index, slot in enumerate(END_SLOTS):
            acc_end[slot, far_end] += product[index * rows:(index + 1) * rows]

    def send_end_parts(index, owner):
        @pl.when(goes(index))
        def _():
            stage_end[index, owner] = acc_end[OFFSETS[index] + 2, owner].astype(BF16)
            part_end_copy(index, owner).start()

    @pl.when(is_mid)
    def _():
        def near_owner(which):
            return jnp.where(which == 0, me, jnp.where(which == 1, other_mid, near_end))

        def multiply(owner, term):
            acc[owner] += jnp.dot(comb[term], blocks[owner, term], preferred_element_type=F32)

        near_three = [me, other_mid, near_end]

        for index, slot in enumerate(END_SLOTS):
            @pl.when(jnp.logical_not(goes(index)))
            def _():
                comb_end[slot] = jnp.zeros(comb_end.shape[1:], BF16)
                comb_extra[slot] = jnp.zeros(comb_extra.shape[1:], BF16)

        state_wait(far_end)
        mask_rows(far_end)

        @pl.when(edge)
        def _():
            @pl.loop(turned, terms)
            def _(term):
                turn_off(term).wait_recv()
                pass_on(term).start()

        @pl.loop(0, terms)
        def _(term):
            blocks[me, term, far_rows, :] = block_of(me, term, far_rows)

        everything = slice(None)

        @pl.loop(0, terms)
        def _(term):
            arrived(other_mid, term)
            blocks[other_mid, term] = block_of(other_mid, term, everything)
            send_block(relay_send, 0, other_mid, term)
            arrived(near_end, term)
            relay_copy(near_end, term, other_mid).start()
            blocks[near_end, term] = block_of(near_end, term, everything)

            @pl.loop(0, 3)
            def _(which):
                multiply(near_owner(which), term)

        @pl.loop(0, 3)
        def _(which):
            send_parts(near_owner(which))

        @pl.loop(0, terms)
        def _(term):
            arrived(far_end, term)
            blocks[far_end, term] = block_of(far_end, term, everything)
            send_block(relay_send, 2, far_end, term)
            multiply(far_end, term)

            for index in range(4):
                slot = OFFSETS[index] + 2

                @pl.when((term == (index + 1) * terms // 4 - 2) & goes(index))
                def _():
                    @pl.loop(cut, terms)
                    def _(late):
                        extra_copy(slot, late, me).wait_recv()
                        extra_multiply(slot, near_three, late)

                    @pl.loop(0, groups)
                    def _(group):
                        end_copy(slot, group, me).wait_recv()

                        end_multiply(slot, group, near_three)

                    @pl.loop(0, 3)
                    def _(which):
                        send_end_parts(index, near_owner(which))

        @pl.loop(cut, terms)
        def _(term):
            add_far(
                [comb_extra[slot, terms - 1 - term] for slot in END_SLOTS],
                blocks[far_end, term, extra_rows, :],
            )

        @pl.loop(0, groups)
        def _(group):
            add_far(
                [end_rows(slot, group, slice(None)) for slot in END_SLOTS],
                far_blocks(far_end, group),
            )

        for index, slot in enumerate(END_SLOTS):
            stage_end[index, far_end] = acc_end[slot, far_end].astype(BF16)

        for first in (True, False):
            for index in range(4):
                @pl.when(goes(index) & (across(index) == first))
                def _():
                    part_end_copy(index, far_end).start()

        send_parts(far_end)

        @pl.loop(cut, terms)
        def _(term):
            extra_copy(home, term, me).wait_recv()
            extra_multiply(home, [0, 1, 2, 3], term)

        def home_strip(part):
            @pl.loop(0, groups)
            def _(group):
                home_copy(part, group, me).wait_recv()

                spot = pl.ds(pl.multiple_of(part * strip, strip), strip)
                end_multiply(home, group, [0, 1, 2, 3], spot)

        def send_back(part):
            spot = pl.ds(pl.multiple_of(part * strip, strip), strip)
            back[:, spot, :] = acc_end[home, :, spot, :].astype(BF16)
            back_copy(part, near_end).start()

        home_strip(0)

        for index in range(4):
            @pl.when(comes(index))
            def _():
                @pl.loop(0, 4)
                def _(owner):
                    part_end_copy(index, owner).wait_recv()
                    acc_end[home, owner] += landed_end[index, owner].astype(F32)

        send_back(0)

        @pl.loop(1, strips)
        def _(part):
            home_strip(part)
            send_back(part)

        @pl.loop(0, 4)
        def _(owner):
            take_parts(owner)
            write_out(owner)

    @pl.when(is_end)
    def _():
        turn = jnp.where(me == 0, 1, -1)
        state_wait(near_mid)
        state_wait(3 - near_mid)

        @pl.loop(0, 3)
        def _(rank):
            mask_rows(me + turn * rank)

        def multiply(owner, term, block, spot):
            acc[owner] += jnp.dot(comb[term, :, spot], block, preferred_element_type=F32)

        @pl.loop(0, cut)
        def _(term):
            multiply(me, term, block_of(me, term, near_rows), near_rows)

        @pl.loop(cut, terms)
        def _(term):
            multiply(me, term, block_of(me, term, short_rows), short_rows)

        send_parts(me)

        @pl.loop(1, 4)
        def _(rank):
            owner = me + turn * rank

            @pl.loop(0, cut)
            def _(term):
                block_arrived(owner, term, near_rows)
                multiply(owner, term, blocks[owner, term, near_rows, :], near_rows)

            @pl.loop(cut, terms)
            def _(term):
                block_arrived(owner, term, short_rows)
                multiply(owner, term, blocks[owner, term, short_rows, :], short_rows)

            send_parts(owner)

        @pl.loop(0, 3)
        def _(rank):
            take_parts(me + turn * rank)

        @pl.loop(0, strips)
        def _(part):
            back_copy(part, me).wait_recv()

        acc[:, home * rows:(home + 1) * rows, :] += back_landed[...].astype(F32)

        @pl.loop(0, 3)
        def _(rank):
            write_out(me + turn * rank)

        take_parts(far_end)
        write_out(far_end)

    for index in range(4):
        @pl.when(goes(index))
        def _():
            @pl.loop(0, 4)
            def _(owner):
                part_copy(index, owner).wait_send()

                @pl.when(is_mid)
                def _():
                    part_end_copy(index, owner).wait_send()

    @pl.when(is_mid)
    def _():
        for part in range(2):
            state_copy(0, me, part, near_end).wait_send()
            state_copy(1, me, part, other_mid).wait_send()
            state_copy(2, other_mid, part, near_end).wait_send()
            state_copy(3, near_end, part, other_mid).wait_send()

        @pl.loop(0, terms)
        def _(term):
            own_copy(term, other_mid).wait_send()
            relay_copy(near_end, term, other_mid).wait_send()
            turns = jnp.logical_not(edge) & (term >= turned)

            @pl.when(turns)
            def _():
                turn_off(term).wait_send()

            @pl.when(edge & (term >= turned))
            def _():
                pass_on(term).wait_send()

            @pl.when(jnp.logical_not(turns))
            def _():
                sent_block(own_send, 1, me, term)

            sent_block(relay_send, 0, other_mid, term)
            sent_block(relay_send, 2, far_end, term)

        @pl.loop(0, strips)
        def _(part):
            back_copy(part, near_end).wait_send()

    @pl.when(is_end)
    def _():
        for part in range(2):
            state_copy(0, me, part, near_mid).wait_send()

        @pl.loop(0, terms)
        def _(term):
            own_copy(term, near_mid).wait_send()

        for index, slot in enumerate(END_SLOTS):
            @pl.when(goes(index))
            def _():
                @pl.loop(cut, terms)
                def _(term):
                    extra_copy(slot, term, near_mid).wait_send()

                @pl.loop(0, groups)
                def _(group):
                    end_copy(slot, group, near_mid).wait_send()

        @pl.loop(cut, terms)
        def _(term):
            extra_copy(home, term, near_mid).wait_send()

        @pl.loop(0, strips)
        def _(part):
            @pl.loop(0, groups)
            def _(group):
                home_copy(part, group, near_mid).wait_send()


def line_apply(sectors, slots, dims, channel_term, channel_out, coefs, state, right, left):
    terms, width, cols = right.shape
    rows = state.shape[0]
    channels = left.shape[0]
    cells = slots * terms
    per = 4
    groups = terms // per
    strips = 2
    detours, extras, least = (2, 5, 0) if sectors == 8 and terms == 16 else (0, 1, 1)
    tall = slots * rows
    dma = pltpu.SemaphoreType.DMA
    any_space = pl.BlockSpec(memory_space=pl.ANY)
    return pl.pallas_call(
        functools.partial(line_kernel, sectors, detours, least),
        out_shape=pltpu.VMEM((rows, width), F32),
        in_specs=[any_space] * 7,
        out_specs=pl.BlockSpec(memory_space=pltpu.VMEM),
        scratch_shapes=[
            pltpu.SMEM(dims.shape, jnp.int32),
            pltpu.VMEM((channels,), jnp.int32),
            pltpu.VMEM((channels,), jnp.int32),
            pltpu.VMEM((channels,), BF16),
            pltpu.VMEM((8, 128), jnp.int32),
            pltpu.SMEM((8, 128), jnp.int32),
            pltpu.VMEM((channels, width), F32),
            pltpu.VMEM((channels, width), F32),
            pltpu.VMEM((cells, width), F32),
            pltpu.VMEM(left.shape, BF16),
            pltpu.VMEM((rows, width), F32),
            pltpu.VMEM(left.shape, BF16),
            pltpu.VMEM((4, rows, width), BF16),
            pltpu.VMEM((width, width), BF16),
            pltpu.VMEM((4, terms, width, cols), BF16),
            pltpu.VMEM((4, terms, width, cols), BF16),
            pltpu.VMEM((terms, tall, width), BF16),
            pltpu.VMEM((slots, groups, per, rows, rows), BF16),
            pltpu.VMEM((slots, extras, rows, rows), BF16),
            pltpu.VMEM((max(detours, 1), width - rows, cols), BF16),
            pltpu.VMEM((4, tall, cols), F32),
            pltpu.VMEM((slots, 4, rows, cols), F32),
            pltpu.VMEM((4, 4, rows, cols), BF16),
            pltpu.VMEM((4, 4, rows, cols), BF16),
            pltpu.VMEM((4, 4, rows, cols), BF16),
            pltpu.VMEM((4, 4, rows, cols), BF16),
            pltpu.VMEM((4, rows, cols), BF16),
            pltpu.VMEM((4, rows, cols), BF16),
            dma((8,)), dma((4, 2)), dma((4, 2)),
            dma((2, terms)), dma((3, terms)), dma((4, terms)),
            dma((slots, groups)), dma((slots, groups)), dma((slots, extras)), dma((slots, extras)),
            dma((strips, groups)), dma((strips, groups)),
            dma((2, max(detours, 1))), dma((max(detours, 1),)),
            dma((4, 4)), dma((4, 4)), dma((4, 4)), dma((4, 4)), dma((2, strips)),
        ],
        compiler_params=pltpu.CompilerParams(
            has_side_effects=True, collective_id=0, vmem_limit_bytes=60 * 2**20
        ),
    )(dims, channel_term, channel_out, coefs, state, right, left)


def passed_along(value, axis, steps):
    count = lax.axis_size(axis)
    first, last = (max(0, -steps), min(count, count - steps))
    return lax.ppermute(value, axis, [(source, source + steps) for source in range(first, last)])


def gathered_apply(sector, live_dim, wave, right, combined, rows, slots):
    width = wave.shape[1]
    terms = right.shape[0]
    whole_state = lax.all_gather(wave, "pan", axis=0, tiled=True)
    indices = lax.iota(jnp.int32, width)
    inside = (indices[:, None] < live_dim) & (indices[None, :] < live_dim)
    masked = jnp.where(inside, whole_state, jnp.zeros((), BF16))
    right_full = lax.all_gather(right, "pan", axis=2, tiled=True)
    term_full = jnp.einsum("ik,wkq->wiq", masked, right_full, preferred_element_type=F32).astype(BF16)
    parts = jnp.einsum(
        "wjri,wiq->jrq", combined.reshape(terms, slots, rows, width), term_full,
        preferred_element_type=F32,
    )
    collected = parts[2]
    for offset in OFFSETS:
        collected = collected + passed_along(parts[offset + 2], "sec", offset)
    return collected


def on_device(
    wave_state, right_blocks, left_blocks, coupling, channel_term, channel_out, sector_dims
):
    rows, width = wave_state.shape[1:]
    terms = right_blocks.shape[1]
    slots = 5
    sector = lax.axis_index("sec")
    live_dim = sector_dims[0]
    if lax.axis_size("pan") == 4 and right_blocks.shape[3] % 128 == 0 and terms % 4 == 0:
        collected = line_apply(
            lax.axis_size("sec"), slots, sector_dims, channel_term, channel_out, coupling,
            wave_state[0], right_blocks[0], left_blocks,
        )
    else:
        cells = channel_term * slots + channel_out - sector + 2
        coefs = coupling.astype(F32)
        combined = combine(cells, coefs, left_blocks, terms * slots)
        collected = gathered_apply(
            sector, live_dim, wave_state[0], right_blocks[0], combined, rows, slots
        )
    indices = lax.iota(jnp.int32, width)
    row_ids = lax.axis_index("pan") * rows + lax.iota(jnp.int32, rows)
    kept_mask = (row_ids[:, None] < live_dim) & (indices[None, :] < live_dim)
    return jnp.where(kept_mask, collected, jnp.zeros((), F32))[None]


def solution(mesh):
    return jax.shard_map(
        on_device,
        mesh=mesh,
        in_specs=(
            P("sec", "pan", None),
            P("sec", None, None, "pan"),
            P("sec", "pan", None),
            P("sec"),
            P("sec"),
            P("sec"),
            P("sec"),
        ),
        out_specs=P("sec", "pan", None),
        check_vma=False,
    )
```

```python
import functools

import jax
import jax.numpy as jnp
from jax import lax
from jax.experimental import pallas as pl
from jax.experimental.pallas import tpu as pltpu
from jax.sharding import PartitionSpec as P

OFFSETS = (-2, -1, 1, 2)
END_SLOTS = (0, 1, 3, 4)
F32 = jnp.float32
BF16 = jnp.bfloat16


def combine_kernel(cell_ref, coef_ref, left_ref, out_ref, acc_ref):
    acc_ref[...] = jnp.zeros_like(acc_ref)

    @pl.loop(0, left_ref.shape[0])
    def _(channel):
        cell = cell_ref[channel]
        acc_ref[cell] += left_ref[channel].astype(F32) * coef_ref[channel]

    @pl.loop(0, out_ref.shape[0])
    def _(cell):
        out_ref[cell] = acc_ref[cell].astype(BF16)


def combine(cells, coefs, left_blocks, cell_count):
    channels, rows, width = left_blocks.shape
    step = min(rows, 32)
    return pl.pallas_call(
        combine_kernel,
        grid=(rows // step,),
        in_specs=[
            pl.BlockSpec(memory_space=pltpu.SMEM),
            pl.BlockSpec(memory_space=pltpu.SMEM),
            pl.BlockSpec((channels, step, width), lambda i: (0, i, 0)),
        ],
        out_specs=pl.BlockSpec((cell_count, step, width), lambda i: (0, i, 0)),
        out_shape=jax.ShapeDtypeStruct((cell_count, rows, width), BF16),
        scratch_shapes=[pltpu.VMEM((cell_count, step, width), F32)],
        compiler_params=pltpu.CompilerParams(vmem_limit_bytes=48 * 2**20),
    )(cells, coefs, left_blocks)


def read_channels(slots, terms, sector, term, out_id, coef, coefs, kept, filled, table):
    count = term.shape[0]
    cells = slots * terms
    width = coefs.shape[1]
    cell = (term[...] * slots + out_id[...] - sector + 2).astype(F32)
    cell_row = jnp.broadcast_to(cell[None, :], (count, count))
    coef_row = jnp.broadcast_to(coef[...].astype(F32)[None, :], (count, count))
    down = lax.broadcasted_iota(jnp.int32, (count, count), 0)
    across = lax.broadcasted_iota(jnp.int32, (count, count), 1)

    def total(mask, values, axis):
        return jnp.sum(jnp.where(mask, values, 0.0), axis=axis, keepdims=True)

    cell_col = total(down == across, cell_row, 1)
    same = cell_col == cell_row
    precedes = (cell_col < cell_row) | (same & (down < across))
    follows = (cell_row < cell_col) | (same & (across < down))
    rank_row = total(precedes, 1.0, 0)
    rank_col = total(follows, 1.0, 1)
    again = jnp.where(total(same & (down < across), 1.0, 0) > 0, 1.0, 0.0)
    spot = rank_row == down.astype(F32)
    coefs[...] = jnp.broadcast_to(total(spot, coef_row, 1), (count, width))
    kept[...] = jnp.broadcast_to(
        total(spot, jnp.broadcast_to(again, (count, count)), 1), (count, width)
    )
    order = total(rank_col == across.astype(F32), down.astype(F32), 0)
    cell_ids = lax.broadcasted_iota(jnp.int32, (count, cells), 1).astype(F32)
    last = total(jnp.broadcast_to(cell_col, (count, cells)) <= cell_ids, 1.0, 0) - 1.0
    ids_down = lax.broadcasted_iota(jnp.int32, (cells, count), 0).astype(F32)
    held = total(ids_down == jnp.broadcast_to(cell[None, :], (cells, count)), 1.0, 1)
    filled[...] = jnp.broadcast_to(jnp.where(held > 0, 1.0, 0.0), (cells, width))
    table[0:1, 0:count] = order.astype(jnp.int32)
    table[1:2, 0:cells] = jnp.maximum(last, 0.0).astype(jnp.int32)


def line_kernel(
    sectors, detours, least, dims_ref, term_ref, out_id_ref, coef_ref, state_ref, right_ref, left_ref,
    out_ref,
    dims, term_ids, out_ids, coef, table, spots, coefs, kept, filled,
    left_all, running, summed,
    state_all, masked, gathered, blocks, comb, comb_end, comb_extra, passing, acc, acc_end,
    stage, landed, stage_end, landed_end, back, back_landed,
    local_sems, state_send, state_recv, own_send, relay_send, right_recv,
    end_send, end_recv, extra_send, extra_recv, home_send, home_recv,
    passing_send, passing_recv, part_send, part_recv, part_end_send, part_end_recv, back_sems,
):
    terms, width, cols = right_ref.shape
    rows = state_ref.shape[0]
    slots = comb.shape[1] // rows
    home = slots // 2
    me = lax.axis_index("pan")
    sector = lax.axis_index("sec")
    is_mid = (me == 1) | (me == 2)
    is_end = jnp.logical_not(is_mid)
    near_end = jnp.where(me <= 1, 0, 3)
    other_mid = jnp.where(me <= 1, 2, 1)
    far_end = 3 - near_end
    near_mid = jnp.where(me <= 1, 1, 2)
    per = comb_end.shape[2]
    groups = terms // per
    edge = (sector < 2) | (sector >= sectors - 2)
    cut = terms - jnp.where(edge, comb_extra.shape[1], least)
    turned = terms - detours
    low = sector < sectors // 2
    outer = jnp.where(low, sector - 2, sector + 2)
    served = jnp.where(low, sector + 2, sector - 2)
    strips = home_send.shape[0]
    strip = rows // strips
    half = rows // 2
    inner = width - rows
    near_rows = pl.ds(pl.multiple_of(jnp.where(near_end == 0, 0, rows), rows), inner)
    far_rows = pl.ds(pl.multiple_of(far_end * rows, rows), rows)
    short_rows = pl.ds(pl.multiple_of(jnp.where(near_end == 0, 0, 2 * rows), rows), inner - rows)
    extra_rows = pl.ds(pl.multiple_of(other_mid * rows, rows), rows)

    def remote(src, dst, send, recv, where, axis="pan"):
        return pltpu.make_async_remote_copy(
            src_ref=src, dst_ref=dst, send_sem=send, recv_sem=recv,
            device_id={axis: where}, device_id_type=pl.DeviceIdType.MESH,
        )

    def state_copy(way, owner, part, where):
        block = state_all.at[owner, pl.ds(part * half, half)]
        return remote(
            block, block, state_send.at[way, part], state_recv.at[owner, part], where
        )

    def state_wait(owner):
        for part in range(2):
            state_copy(0, owner, part, me).wait_recv()

    def own_copy(term, where):
        return remote(
            right_ref.at[term], gathered.at[me, term],
            own_send.at[0, term], right_recv.at[me, term], where,
        )

    def relay_copy(owner, term, where):
        block = gathered.at[owner, term]
        return remote(block, block, relay_send.at[1, term], right_recv.at[owner, term], where)

    def block_copy(sems, way, owner, term, where, spot):
        block = blocks.at[owner, term, spot]
        return remote(block, block, sems.at[way, term], right_recv.at[owner, term], where)

    def send_block(sems, way, owner, term):
        @pl.when(term < cut)
        def _():
            block_copy(sems, way, owner, term, near_end, near_rows).start()

        @pl.when(term >= cut)
        def _():
            block_copy(sems, way, owner, term, near_end, short_rows).start()

    def sent_block(sems, way, owner, term):
        @pl.when(term < cut)
        def _():
            block_copy(sems, way, owner, term, near_end, near_rows).wait_send()

        @pl.when(term >= cut)
        def _():
            block_copy(sems, way, owner, term, near_end, short_rows).wait_send()

    def turn_off(term):
        index = term - turned
        return remote(
            blocks.at[me, term, near_rows], passing.at[index],
            passing_send.at[0, index], passing_recv.at[index], outer, "sec",
        )

    def pass_on(term):
        index = term - turned
        return pltpu.make_async_remote_copy(
            src_ref=passing.at[index], dst_ref=blocks.at[me, term, near_rows],
            send_sem=passing_send.at[1, index], recv_sem=right_recv.at[me, term],
            device_id={"sec": served, "pan": near_end}, device_id_type=pl.DeviceIdType.MESH,
        )

    def block_arrived(owner, term, spot):
        block_copy(relay_send, 0, owner, term, me, spot).wait_recv()

    def end_copy(slot, group, where):
        spot = pl.ds(pl.multiple_of(slot * rows, rows), rows)
        return remote(
            comb.at[pl.ds(group * per, per), spot, far_rows], comb_end.at[slot, group],
            end_send.at[slot, group], end_recv.at[slot, group], where,
        )

    def extra_copy(slot, term, where):
        spot = pl.ds(pl.multiple_of(slot * rows, rows), rows)
        index = terms - 1 - term
        return remote(
            comb.at[term, spot, extra_rows], comb_extra.at[slot, index],
            extra_send.at[slot, index], extra_recv.at[slot, index], where,
        )

    def home_copy(part, group, where):
        source = pl.ds(home * rows + part * strip, strip)
        spot = pl.ds(part * strip, strip)
        return remote(
            comb.at[pl.ds(group * per, per), source, far_rows], comb_end.at[home, group, :, spot],
            home_send.at[part, group], home_recv.at[part, group], where,
        )

    def arrived(owner, term):
        block = gathered.at[owner, term]
        remote(block, block, relay_send.at[0, term], right_recv.at[owner, term], me).wait_recv()

    def part_copy(index, owner):
        return remote(
            stage.at[index, owner], landed.at[index, owner],
            part_send.at[index, owner], part_recv.at[index, owner], sector + OFFSETS[index], "sec",
        )

    def part_end_copy(index, owner):
        return remote(
            stage_end.at[index, owner], landed_end.at[index, owner],
            part_end_send.at[index, owner], part_end_recv.at[index, owner],
            sector + OFFSETS[index], "sec",
        )

    def back_copy(part, where):
        spot = pl.ds(part * strip, strip)
        return remote(
            back.at[:, spot], back_landed.at[:, spot],
            back_sems.at[0, part], back_sems.at[1, part], where,
        )

    def goes(index):
        target = sector + OFFSETS[index]
        return (target >= 0) & (target < sectors)

    def comes(index):
        source = sector - OFFSETS[index]
        return (source >= 0) & (source < sectors)

    small = [
        pltpu.make_async_copy(dims_ref, dims, local_sems.at[0]),
        pltpu.make_async_copy(term_ref, term_ids, local_sems.at[1]),
        pltpu.make_async_copy(out_id_ref, out_ids, local_sems.at[2]),
        pltpu.make_async_copy(coef_ref, coef, local_sems.at[3]),
    ]
    large = [
        pltpu.make_async_copy(left_ref, left_all, local_sems.at[4]),
        pltpu.make_async_copy(state_ref, state_all.at[me], local_sems.at[5]),
        pltpu.make_async_copy(right_ref, gathered.at[me], local_sems.at[6]),
    ]
    for copy in large[1:2] + small + large[2:] + large[:1]:
        copy.start()

    barrier = pltpu.get_barrier_semaphore()

    def greet(axis, where):
        pl.semaphore_signal(
            barrier, inc=1, device_id={axis: where}, device_id_type=pl.DeviceIdType.MESH
        )

    greet("pan", jnp.where(is_mid, near_end, near_mid))

    @pl.when(is_mid)
    def _():
        greet("pan", other_mid)

    peers = jnp.where(is_mid, 2, 1)
    for index in range(4):
        peers = peers + goes(index).astype(jnp.int32)

        @pl.when(goes(index))
        def _():
            greet("sec", sector + OFFSETS[index])

    pl.semaphore_wait(barrier, peers)

    large[1].wait()

    @pl.when(is_mid)
    def _():
        for part in range(2):
            state_copy(0, me, part, near_end).start()
            state_copy(1, me, part, other_mid).start()

        @pl.loop(0, 2)
        def _(term):
            own_copy(term, other_mid).start()

    @pl.when(is_end)
    def _():
        for part in range(2):
            state_copy(0, me, part, near_mid).start()

        @pl.loop(0, terms)
        def _(term):
            own_copy(term, near_mid).start()

    for copy in small:
        copy.wait()
    read_channels(slots, terms, sector, term_ids, out_ids, coef, coefs, kept, filled, table)
    spots_copy = pltpu.make_async_copy(table, spots, local_sems.at[7])
    spots_copy.start()
    acc[...] = jnp.zeros_like(acc)
    acc_end[...] = jnp.zeros_like(acc_end)
    running[...] = jnp.zeros_like(running)

    live = dims[0]
    inside_col = lax.broadcasted_iota(jnp.int32, (rows, width), 1) < live

    def mask_rows(owner):
        row = lax.broadcasted_iota(jnp.int32, (rows, width), 0) + owner * rows
        spot = pl.ds(pl.multiple_of(owner * rows, rows), rows)
        masked[spot, :] = jnp.where(
            inside_col & (row < live), state_all[owner].astype(F32), 0.0
        ).astype(BF16)

    def block_of(owner, term, spot):
        return jnp.dot(
            masked[spot, :], gathered[owner, term], preferred_element_type=F32
        ).astype(BF16)

    large[2].wait()

    @pl.when(is_mid)
    def _():
        for part in range(2):
            state_copy(0, other_mid, part, me).wait_recv()
            state_copy(2, other_mid, part, near_end).start()
            state_copy(0, near_end, part, me).wait_recv()
            state_copy(3, near_end, part, other_mid).start()

        @pl.loop(2, terms)
        def _(term):
            own_copy(term, other_mid).start()

        @pl.loop(0, 3)
        def _(which):
            mask_rows(jnp.where(which == 0, me, jnp.where(which == 1, other_mid, near_end)))

        @pl.loop(0, terms)
        def _(term):
            blocks[me, term, near_rows, :] = block_of(me, term, near_rows)
            turns = jnp.logical_not(edge) & (term >= turned)

            @pl.when(turns)
            def _():
                turn_off(term).start()

            @pl.when(jnp.logical_not(turns))
            def _():
                send_block(own_send, 1, me, term)

    spots_copy.wait()
    large[0].wait()
    channels = left_all.shape[0]

    def inside(spot):
        return jnp.minimum(jnp.maximum(spot, 0), channels - 1)

    @pl.loop(0, channels)
    def _(step):
        row = pl.ds(step, 1)
        total = running[...] * kept[row, :] + left_all[inside(spots[0, step])].astype(F32) * coefs[row, :]
        running[...] = total
        summed[step] = total.astype(BF16)

    @pl.loop(0, terms)
    def _(term):
        for slot in range(slots):
            cell = term * slots + slot
            value = summed[inside(spots[1, cell])].astype(F32) * filled[pl.ds(cell, 1), :]
            comb[term, slot * rows:(slot + 1) * rows, :] = value.astype(BF16)

    @pl.when(is_end)
    def _():
        for index, slot in enumerate(END_SLOTS):
            @pl.when(goes(index))
            def _():
                @pl.loop(cut, terms)
                def _(term):
                    extra_copy(slot, term, near_mid).start()

                @pl.loop(0, groups)
                def _(group):
                    end_copy(slot, group, near_mid).start()

        @pl.loop(cut, terms)
        def _(term):
            extra_copy(home, term, near_mid).start()

        @pl.loop(0, strips)
        def _(part):
            @pl.loop(0, groups)
            def _(group):
                home_copy(part, group, near_mid).start()

    def across(index):
        return (sector // 2 + (sector + OFFSETS[index]) // 2) % 4 == 3

    def send_parts(owner):
        for index, slot in enumerate(END_SLOTS):
            stage[index, owner] = acc[owner, slot * rows:(slot + 1) * rows, :].astype(BF16)

        for first in (True, False):
            for index in range(4):
                @pl.when(goes(index) & (across(index) == first))
                def _():
                    part_copy(index, owner).start()

    def take_parts(owner):
        for index in range(4):
            @pl.when(comes(index))
            def _():
                part_copy(index, owner).wait_recv()
                acc[owner, home * rows:(home + 1) * rows, :] += landed[index, owner].astype(F32)

    def write_out(owner):
        for spot in range(4):
            @pl.when(owner == spot)
            def _():
                out_ref[:, spot * cols:(spot + 1) * cols] = acc[spot, home * rows:(home + 1) * rows, :]

    def far_blocks(owner, group):
        return jnp.concatenate(
            [blocks[owner, group * per + index, far_rows, :] for index in range(per)], axis=0
        )

    def end_rows(slot, group, spot):
        return jnp.concatenate(
            [comb_end[slot, group, index, spot, :] for index in range(per)], axis=1
        )

    def add_end(slot, owners, spot, left, rights):
        for first in range(0, len(owners), 2):
            pair = owners[first:first + 2]
            product = jnp.dot(
                left, jnp.concatenate(rights[first:first + 2], axis=1), preferred_element_type=F32
            )
            for index, owner in enumerate(pair):
                acc_end[slot, owner, spot, :] += product[:, index * cols:(index + 1) * cols]

    def end_multiply(slot, group, owners, spot=slice(None)):
        rights = [far_blocks(owner, group) for owner in owners]
        add_end(slot, owners, spot, end_rows(slot, group, spot), rights)

    extras = comb_extra.shape[1]
    has_extras = edge | (least > 0)

    def extra_left(slot):
        return jnp.concatenate([comb_extra[slot, index] for index in range(extras)], axis=1)

    def extra_right(owner):
        return jnp.concatenate(
            [blocks[owner, terms - 1 - index, extra_rows, :] for index in range(extras)], axis=0
        )

    def extra_multiply(slot, owners):
        @pl.loop(cut, terms)
        def _(term):
            extra_copy(slot, term, me).wait_recv()

        @pl.when(has_extras)
        def _():
            rights = [extra_right(owner) for owner in owners]
            add_end(slot, owners, slice(None), extra_left(slot), rights)

    def add_far(left, right):
        product = jnp.dot(
            jnp.concatenate(left, axis=0), right, preferred_element_type=F32
        )
        for index, slot in enumerate(END_SLOTS):
            acc_end[slot, far_end] += product[index * rows:(index + 1) * rows]

    def send_end_parts(index, owner):
        @pl.when(goes(index))
        def _():
            stage_end[index, owner] = acc_end[OFFSETS[index] + 2, owner].astype(BF16)
            part_end_copy(index, owner).start()

    @pl.when(is_mid)
    def _():
        def near_owner(which):
            return jnp.where(which == 0, me, jnp.where(which == 1, other_mid, near_end))

        def multiply(owner, term):
            acc[owner] += jnp.dot(comb[term], blocks[owner, term], preferred_element_type=F32)

        near_three = [me, other_mid, near_end]

        def add_far_group(group):
            add_far(
                [end_rows(slot, group, slice(None)) for slot in END_SLOTS],
                far_blocks(far_end, group),
            )

        for index, slot in enumerate(END_SLOTS):
            @pl.when(jnp.logical_not(goes(index)))
            def _():
                comb_end[slot] = jnp.zeros(comb_end.shape[1:], BF16)
                comb_extra[slot] = jnp.zeros(comb_extra.shape[1:], BF16)

        state_wait(far_end)
        mask_rows(far_end)

        @pl.when(edge)
        def _():
            @pl.loop(turned, terms)
            def _(term):
                turn_off(term).wait_recv()
                pass_on(term).start()

        @pl.loop(0, terms)
        def _(term):
            blocks[me, term, far_rows, :] = block_of(me, term, far_rows)

        everything = slice(None)

        @pl.loop(0, terms)
        def _(term):
            arrived(other_mid, term)
            blocks[other_mid, term] = block_of(other_mid, term, everything)
            send_block(relay_send, 0, other_mid, term)
            arrived(near_end, term)
            relay_copy(near_end, term, other_mid).start()
            blocks[near_end, term] = block_of(near_end, term, everything)

            @pl.loop(0, 3)
            def _(which):
                multiply(near_owner(which), term)

        @pl.loop(0, 3)
        def _(which):
            send_parts(near_owner(which))

        @pl.loop(0, terms)
        def _(term):
            arrived(far_end, term)
            blocks[far_end, term] = block_of(far_end, term, everything)
            send_block(relay_send, 2, far_end, term)

            @pl.when(term < terms - 1)
            def _():
                multiply(far_end, term)

            for index in range(4):
                slot = OFFSETS[index] + 2

                @pl.when((term == (index + 1) * terms // 4 - 2) & goes(index))
                def _():
                    extra_multiply(slot, near_three)

                    @pl.loop(0, groups)
                    def _(group):
                        end_copy(slot, group, me).wait_recv()

                        end_multiply(slot, group, near_three)

                    @pl.loop(0, 3)
                    def _(which):
                        send_end_parts(index, near_owner(which))

            @pl.when(term == terms - 2)
            def _():
                @pl.loop(0, groups - 1)
                def _(group):
                    add_far_group(group)

        add_far_group(groups - 1)

        @pl.when(has_extras)
        def _():
            add_far([extra_left(slot) for slot in END_SLOTS], extra_right(far_end))

        for index, slot in enumerate(END_SLOTS):
            stage_end[index, far_end] = acc_end[slot, far_end].astype(BF16)

        for first in (True, False):
            for index in range(4):
                @pl.when(goes(index) & (across(index) == first))
                def _():
                    part_end_copy(index, far_end).start()

        multiply(far_end, terms - 1)

        extra_multiply(home, [0, 1, 2, 3])

        def home_strip(part):
            @pl.loop(0, groups)
            def _(group):
                home_copy(part, group, me).wait_recv()

                spot = pl.ds(pl.multiple_of(part * strip, strip), strip)
                end_multiply(home, group, [0, 1, 2, 3], spot)

        def send_back(part):
            spot = pl.ds(pl.multiple_of(part * strip, strip), strip)
            back[:, spot, :] = acc_end[home, :, spot, :].astype(BF16)
            back_copy(part, near_end).start()

        home_strip(0)

        for index in range(4):
            @pl.when(comes(index))
            def _():
                @pl.loop(0, 4)
                def _(owner):
                    part_end_copy(index, owner).wait_recv()
                    acc_end[home, owner] += landed_end[index, owner].astype(F32)

        send_back(0)
        send_parts(far_end)

        @pl.loop(1, strips)
        def _(part):
            home_strip(part)
            send_back(part)

        @pl.loop(0, 4)
        def _(owner):
            take_parts(owner)
            write_out(owner)

    @pl.when(is_end)
    def _():
        turn = jnp.where(me == 0, 1, -1)
        state_wait(near_mid)
        state_wait(3 - near_mid)

        @pl.loop(0, 3)
        def _(rank):
            mask_rows(me + turn * rank)

        def multiply(owner, term, block, spot):
            acc[owner] += jnp.dot(comb[term, :, spot], block, preferred_element_type=F32)

        @pl.loop(0, cut)
        def _(term):
            multiply(me, term, block_of(me, term, near_rows), near_rows)

        @pl.loop(cut, terms)
        def _(term):
            multiply(me, term, block_of(me, term, short_rows), short_rows)

        send_parts(me)

        @pl.loop(1, 4)
        def _(rank):
            owner = me + turn * rank

            @pl.loop(0, cut)
            def _(term):
                block_arrived(owner, term, near_rows)
                multiply(owner, term, blocks[owner, term, near_rows, :], near_rows)

            @pl.loop(cut, terms)
            def _(term):
                block_arrived(owner, term, short_rows)
                multiply(owner, term, blocks[owner, term, short_rows, :], short_rows)

            send_parts(owner)

        @pl.loop(0, 3)
        def _(rank):
            take_parts(me + turn * rank)

        @pl.loop(0, strips)
        def _(part):
            back_copy(part, me).wait_recv()

        acc[:, home * rows:(home + 1) * rows, :] += back_landed[...].astype(F32)

        @pl.loop(0, 3)
        def _(rank):
            write_out(me + turn * rank)

        take_parts(far_end)
        write_out(far_end)

    for index in range(4):
        @pl.when(goes(index))
        def _():
            @pl.loop(0, 4)
            def _(owner):
                part_copy(index, owner).wait_send()

                @pl.when(is_mid)
                def _():
                    part_end_copy(index, owner).wait_send()

    @pl.when(is_mid)
    def _():
        for part in range(2):
            state_copy(0, me, part, near_end).wait_send()
            state_copy(1, me, part, other_mid).wait_send()
            state_copy(2, other_mid, part, near_end).wait_send()
            state_copy(3, near_end, part, other_mid).wait_send()

        @pl.loop(0, terms)
        def _(term):
            own_copy(term, other_mid).wait_send()
            relay_copy(near_end, term, other_mid).wait_send()
            turns = jnp.logical_not(edge) & (term >= turned)

            @pl.when(turns)
            def _():
                turn_off(term).wait_send()

            @pl.when(edge & (term >= turned))
            def _():
                pass_on(term).wait_send()

            @pl.when(jnp.logical_not(turns))
            def _():
                sent_block(own_send, 1, me, term)

            sent_block(relay_send, 0, other_mid, term)
            sent_block(relay_send, 2, far_end, term)

        @pl.loop(0, strips)
        def _(part):
            back_copy(part, near_end).wait_send()

    @pl.when(is_end)
    def _():
        for part in range(2):
            state_copy(0, me, part, near_mid).wait_send()

        @pl.loop(0, terms)
        def _(term):
            own_copy(term, near_mid).wait_send()

        for index, slot in enumerate(END_SLOTS):
            @pl.when(goes(index))
            def _():
                @pl.loop(cut, terms)
                def _(term):
                    extra_copy(slot, term, near_mid).wait_send()

                @pl.loop(0, groups)
                def _(group):
                    end_copy(slot, group, near_mid).wait_send()

        @pl.loop(cut, terms)
        def _(term):
            extra_copy(home, term, near_mid).wait_send()

        @pl.loop(0, strips)
        def _(part):
            @pl.loop(0, groups)
            def _(group):
                home_copy(part, group, near_mid).wait_send()


def line_apply(sectors, slots, dims, channel_term, channel_out, coefs, state, right, left):
    terms, width, cols = right.shape
    rows = state.shape[0]
    channels = left.shape[0]
    cells = slots * terms
    per = 4
    groups = terms // per
    strips = 2
    detours, extras, least = (3, 6, 0) if sectors == 8 and terms == 16 else (0, 1, 1)
    tall = slots * rows
    dma = pltpu.SemaphoreType.DMA
    any_space = pl.BlockSpec(memory_space=pl.ANY)
    return pl.pallas_call(
        functools.partial(line_kernel, sectors, detours, least),
        out_shape=pltpu.VMEM((rows, width), F32),
        in_specs=[any_space] * 7,
        out_specs=pl.BlockSpec(memory_space=pltpu.VMEM),
        scratch_shapes=[
            pltpu.SMEM(dims.shape, jnp.int32),
            pltpu.VMEM((channels,), jnp.int32),
            pltpu.VMEM((channels,), jnp.int32),
            pltpu.VMEM((channels,), BF16),
            pltpu.VMEM((8, 128), jnp.int32),
            pltpu.SMEM((8, 128), jnp.int32),
            pltpu.VMEM((channels, width), F32),
            pltpu.VMEM((channels, width), F32),
            pltpu.VMEM((cells, width), F32),
            pltpu.VMEM(left.shape, BF16),
            pltpu.VMEM((rows, width), F32),
            pltpu.VMEM(left.shape, BF16),
            pltpu.VMEM((4, rows, width), BF16),
            pltpu.VMEM((width, width), BF16),
            pltpu.VMEM((4, terms, width, cols), BF16),
            pltpu.VMEM((4, terms, width, cols), BF16),
            pltpu.VMEM((terms, tall, width), BF16),
            pltpu.VMEM((slots, groups, per, rows, rows), BF16),
            pltpu.VMEM((slots, extras, rows, rows), BF16),
            pltpu.VMEM((max(detours, 1), width - rows, cols), BF16),
            pltpu.VMEM((4, tall, cols), F32),
            pltpu.VMEM((slots, 4, rows, cols), F32),
            pltpu.VMEM((4, 4, rows, cols), BF16),
            pltpu.VMEM((4, 4, rows, cols), BF16),
            pltpu.VMEM((4, 4, rows, cols), BF16),
            pltpu.VMEM((4, 4, rows, cols), BF16),
            pltpu.VMEM((4, rows, cols), BF16),
            pltpu.VMEM((4, rows, cols), BF16),
            dma((8,)), dma((4, 2)), dma((4, 2)),
            dma((2, terms)), dma((3, terms)), dma((4, terms)),
            dma((slots, groups)), dma((slots, groups)), dma((slots, extras)), dma((slots, extras)),
            dma((strips, groups)), dma((strips, groups)),
            dma((2, max(detours, 1))), dma((max(detours, 1),)),
            dma((4, 4)), dma((4, 4)), dma((4, 4)), dma((4, 4)), dma((2, strips)),
        ],
        compiler_params=pltpu.CompilerParams(
            has_side_effects=True, collective_id=0, vmem_limit_bytes=60 * 2**20
        ),
    )(dims, channel_term, channel_out, coefs, state, right, left)


def passed_along(value, axis, steps):
    count = lax.axis_size(axis)
    first, last = (max(0, -steps), min(count, count - steps))
    return lax.ppermute(value, axis, [(source, source + steps) for source in range(first, last)])


def gathered_apply(sector, live_dim, wave, right, combined, rows, slots):
    width = wave.shape[1]
    terms = right.shape[0]
    whole_state = lax.all_gather(wave, "pan", axis=0, tiled=True)
    indices = lax.iota(jnp.int32, width)
    inside = (indices[:, None] < live_dim) & (indices[None, :] < live_dim)
    masked = jnp.where(inside, whole_state, jnp.zeros((), BF16))
    right_full = lax.all_gather(right, "pan", axis=2, tiled=True)
    term_full = jnp.einsum("ik,wkq->wiq", masked, right_full, preferred_element_type=F32).astype(BF16)
    parts = jnp.einsum(
        "wjri,wiq->jrq", combined.reshape(terms, slots, rows, width), term_full,
        preferred_element_type=F32,
    )
    collected = parts[2]
    for offset in OFFSETS:
        collected = collected + passed_along(parts[offset + 2], "sec", offset)
    return collected


def on_device(
    wave_state, right_blocks, left_blocks, coupling, channel_term, channel_out, sector_dims
):
    rows, width = wave_state.shape[1:]
    terms = right_blocks.shape[1]
    slots = 5
    sector = lax.axis_index("sec")
    live_dim = sector_dims[0]
    if lax.axis_size("pan") == 4 and right_blocks.shape[3] % 128 == 0 and terms % 4 == 0:
        collected = line_apply(
            lax.axis_size("sec"), slots, sector_dims, channel_term, channel_out, coupling,
            wave_state[0], right_blocks[0], left_blocks,
        )
    else:
        cells = channel_term * slots + channel_out - sector + 2
        coefs = coupling.astype(F32)
        combined = combine(cells, coefs, left_blocks, terms * slots)
        collected = gathered_apply(
            sector, live_dim, wave_state[0], right_blocks[0], combined, rows, slots
        )
    indices = lax.iota(jnp.int32, width)
    row_ids = lax.axis_index("pan") * rows + lax.iota(jnp.int32, rows)
    kept_mask = (row_ids[:, None] < live_dim) & (indices[None, :] < live_dim)
    return jnp.where(kept_mask, collected, jnp.zeros((), F32))[None]


def solution(mesh):
    return jax.shard_map(
        on_device,
        mesh=mesh,
        in_specs=(
            P("sec", "pan", None),
            P("sec", None, None, "pan"),
            P("sec", "pan", None),
            P("sec"),
            P("sec"),
            P("sec"),
            P("sec"),
        ),
        out_specs=P("sec", "pan", None),
        check_vma=False,
    )
```

```python
import functools

import jax
import jax.numpy as jnp
from jax import lax
from jax.experimental import pallas as pl
from jax.experimental.pallas import tpu as pltpu
from jax.sharding import PartitionSpec as P

OFFSETS = (-2, -1, 1, 2)
END_SLOTS = (0, 1, 3, 4)
F32 = jnp.float32
BF16 = jnp.bfloat16


def combine_kernel(cell_ref, coef_ref, left_ref, out_ref, acc_ref):
    acc_ref[...] = jnp.zeros_like(acc_ref)

    @pl.loop(0, left_ref.shape[0])
    def _(channel):
        cell = cell_ref[channel]
        acc_ref[cell] += left_ref[channel].astype(F32) * coef_ref[channel]

    @pl.loop(0, out_ref.shape[0])
    def _(cell):
        out_ref[cell] = acc_ref[cell].astype(BF16)


def combine(cells, coefs, left_blocks, cell_count):
    channels, rows, width = left_blocks.shape
    step = min(rows, 32)
    return pl.pallas_call(
        combine_kernel,
        grid=(rows // step,),
        in_specs=[
            pl.BlockSpec(memory_space=pltpu.SMEM),
            pl.BlockSpec(memory_space=pltpu.SMEM),
            pl.BlockSpec((channels, step, width), lambda i: (0, i, 0)),
        ],
        out_specs=pl.BlockSpec((cell_count, step, width), lambda i: (0, i, 0)),
        out_shape=jax.ShapeDtypeStruct((cell_count, rows, width), BF16),
        scratch_shapes=[pltpu.VMEM((cell_count, step, width), F32)],
        compiler_params=pltpu.CompilerParams(vmem_limit_bytes=48 * 2**20),
    )(cells, coefs, left_blocks)


def read_channels(slots, terms, sector, term, out_id, coef, coefs, kept, filled, table):
    count = term.shape[0]
    cells = slots * terms
    width = coefs.shape[1]
    cell = (term[...] * slots + out_id[...] - sector + 2).astype(F32)
    cell_row = jnp.broadcast_to(cell[None, :], (count, count))
    coef_row = jnp.broadcast_to(coef[...].astype(F32)[None, :], (count, count))
    down = lax.broadcasted_iota(jnp.int32, (count, count), 0)
    across = lax.broadcasted_iota(jnp.int32, (count, count), 1)

    def total(mask, values, axis):
        return jnp.sum(jnp.where(mask, values, 0.0), axis=axis, keepdims=True)

    cell_col = total(down == across, cell_row, 1)
    same = cell_col == cell_row
    precedes = (cell_col < cell_row) | (same & (down < across))
    follows = (cell_row < cell_col) | (same & (across < down))
    rank_row = total(precedes, 1.0, 0)
    rank_col = total(follows, 1.0, 1)
    again = jnp.where(total(same & (down < across), 1.0, 0) > 0, 1.0, 0.0)
    spot = rank_row == down.astype(F32)
    coefs[...] = jnp.broadcast_to(total(spot, coef_row, 1), (count, width))
    kept[...] = jnp.broadcast_to(
        total(spot, jnp.broadcast_to(again, (count, count)), 1), (count, width)
    )
    order = total(rank_col == across.astype(F32), down.astype(F32), 0)
    cell_ids = lax.broadcasted_iota(jnp.int32, (count, cells), 1).astype(F32)
    last = total(jnp.broadcast_to(cell_col, (count, cells)) <= cell_ids, 1.0, 0) - 1.0
    ids_down = lax.broadcasted_iota(jnp.int32, (cells, count), 0).astype(F32)
    held = total(ids_down == jnp.broadcast_to(cell[None, :], (cells, count)), 1.0, 1)
    filled[...] = jnp.broadcast_to(jnp.where(held > 0, 1.0, 0.0), (cells, width))
    table[0:1, 0:count] = order.astype(jnp.int32)
    table[1:2, 0:cells] = jnp.maximum(last, 0.0).astype(jnp.int32)


def line_kernel(
    sectors, detours, least, dims_ref, term_ref, out_id_ref, coef_ref, state_ref, right_ref, left_ref,
    out_ref,
    dims, term_ids, out_ids, coef, table, spots, coefs, kept, filled,
    left_all, running, summed,
    state_all, masked, gathered, blocks, comb, comb_end, comb_extra, passing, acc, acc_end,
    stage, landed, stage_end, landed_end, back, back_landed,
    local_sems, state_send, state_recv, own_send, relay_send, right_recv,
    end_send, end_recv, extra_send, extra_recv, home_send, home_recv,
    passing_send, passing_recv, part_send, part_recv, part_end_send, part_end_recv, back_sems,
):
    terms, width, cols = right_ref.shape
    rows = state_ref.shape[0]
    slots = comb.shape[1] // rows
    home = slots // 2
    me = lax.axis_index("pan")
    sector = lax.axis_index("sec")
    is_mid = (me == 1) | (me == 2)
    is_end = jnp.logical_not(is_mid)
    near_end = jnp.where(me <= 1, 0, 3)
    other_mid = jnp.where(me <= 1, 2, 1)
    far_end = 3 - near_end
    near_mid = jnp.where(me <= 1, 1, 2)
    per = comb_end.shape[2]
    groups = terms // per
    edge = (sector < 2) | (sector >= sectors - 2)
    cut = terms - jnp.where(edge, comb_extra.shape[1], least)
    turned = terms - detours
    low = sector < sectors // 2
    outer = jnp.where(low, sector - 2, sector + 2)
    served = jnp.where(low, sector + 2, sector - 2)
    strips = home_send.shape[0]
    strip = rows // strips
    half = rows // 2
    inner = width - rows
    near_rows = pl.ds(pl.multiple_of(jnp.where(near_end == 0, 0, rows), rows), inner)
    far_rows = pl.ds(pl.multiple_of(far_end * rows, rows), rows)
    short_rows = pl.ds(pl.multiple_of(jnp.where(near_end == 0, 0, 2 * rows), rows), inner - rows)
    extra_rows = pl.ds(pl.multiple_of(other_mid * rows, rows), rows)

    def remote(src, dst, send, recv, where, axis="pan"):
        return pltpu.make_async_remote_copy(
            src_ref=src, dst_ref=dst, send_sem=send, recv_sem=recv,
            device_id={axis: where}, device_id_type=pl.DeviceIdType.MESH,
        )

    def state_copy(way, owner, part, where):
        block = state_all.at[owner, pl.ds(part * half, half)]
        return remote(
            block, block, state_send.at[way, part], state_recv.at[owner, part], where
        )

    def state_wait(owner):
        for part in range(2):
            state_copy(0, owner, part, me).wait_recv()

    def own_copy(term, where):
        return remote(
            right_ref.at[term], gathered.at[me, term],
            own_send.at[0, term], right_recv.at[me, term], where,
        )

    def relay_copy(owner, term, where):
        block = gathered.at[owner, term]
        return remote(block, block, relay_send.at[1, term], right_recv.at[owner, term], where)

    def block_copy(sems, way, owner, term, where, spot):
        block = blocks.at[owner, term, spot]
        return remote(block, block, sems.at[way, term], right_recv.at[owner, term], where)

    def send_block(sems, way, owner, term):
        @pl.when(term < cut)
        def _():
            block_copy(sems, way, owner, term, near_end, near_rows).start()

        @pl.when(term >= cut)
        def _():
            block_copy(sems, way, owner, term, near_end, short_rows).start()

    def sent_block(sems, way, owner, term):
        @pl.when(term < cut)
        def _():
            block_copy(sems, way, owner, term, near_end, near_rows).wait_send()

        @pl.when(term >= cut)
        def _():
            block_copy(sems, way, owner, term, near_end, short_rows).wait_send()

    def turn_off(term):
        index = term - turned
        return remote(
            blocks.at[me, term, near_rows], passing.at[index],
            passing_send.at[0, index], passing_recv.at[index], outer, "sec",
        )

    def pass_on(term):
        index = term - turned
        return pltpu.make_async_remote_copy(
            src_ref=passing.at[index], dst_ref=blocks.at[me, term, near_rows],
            send_sem=passing_send.at[1, index], recv_sem=right_recv.at[me, term],
            device_id={"sec": served, "pan": near_end}, device_id_type=pl.DeviceIdType.MESH,
        )

    def block_arrived(owner, term, spot):
        block_copy(relay_send, 0, owner, term, me, spot).wait_recv()

    def end_copy(slot, group, where):
        spot = pl.ds(pl.multiple_of(slot * rows, rows), rows)
        return remote(
            comb.at[pl.ds(group * per, per), spot, far_rows], comb_end.at[slot, group],
            end_send.at[slot, group], end_recv.at[slot, group], where,
        )

    def extra_copy(slot, term, where):
        spot = pl.ds(pl.multiple_of(slot * rows, rows), rows)
        index = terms - 1 - term
        return remote(
            comb.at[term, spot, extra_rows], comb_extra.at[slot, index],
            extra_send.at[slot, index], extra_recv.at[slot, index], where,
        )

    def home_copy(part, group, where):
        source = pl.ds(home * rows + part * strip, strip)
        spot = pl.ds(part * strip, strip)
        return remote(
            comb.at[pl.ds(group * per, per), source, far_rows], comb_end.at[home, group, :, spot],
            home_send.at[part, group], home_recv.at[part, group], where,
        )

    def arrived(owner, term):
        block = gathered.at[owner, term]
        remote(block, block, relay_send.at[0, term], right_recv.at[owner, term], me).wait_recv()

    def part_copy(index, owner):
        return remote(
            stage.at[index, owner], landed.at[index, owner],
            part_send.at[index, owner], part_recv.at[index, owner], sector + OFFSETS[index], "sec",
        )

    def part_end_copy(index, owner):
        return remote(
            stage_end.at[index, owner], landed_end.at[index, owner],
            part_end_send.at[index, owner], part_end_recv.at[index, owner],
            sector + OFFSETS[index], "sec",
        )

    def back_copy(part, where):
        spot = pl.ds(part * strip, strip)
        return remote(
            back.at[:, spot], back_landed.at[:, spot],
            back_sems.at[0, part], back_sems.at[1, part], where,
        )

    def goes(index):
        target = sector + OFFSETS[index]
        return (target >= 0) & (target < sectors)

    def comes(index):
        source = sector - OFFSETS[index]
        return (source >= 0) & (source < sectors)

    small = [
        pltpu.make_async_copy(dims_ref, dims, local_sems.at[0]),
        pltpu.make_async_copy(term_ref, term_ids, local_sems.at[1]),
        pltpu.make_async_copy(out_id_ref, out_ids, local_sems.at[2]),
        pltpu.make_async_copy(coef_ref, coef, local_sems.at[3]),
    ]
    large = [
        pltpu.make_async_copy(left_ref, left_all, local_sems.at[4]),
        pltpu.make_async_copy(state_ref, state_all.at[me], local_sems.at[5]),
        pltpu.make_async_copy(right_ref, gathered.at[me], local_sems.at[6]),
    ]
    for copy in large[1:2] + small + large[2:] + large[:1]:
        copy.start()

    barrier = pltpu.get_barrier_semaphore()

    def greet(axis, where):
        pl.semaphore_signal(
            barrier, inc=1, device_id={axis: where}, device_id_type=pl.DeviceIdType.MESH
        )

    greet("pan", jnp.where(is_mid, near_end, near_mid))

    @pl.when(is_mid)
    def _():
        greet("pan", other_mid)

    peers = jnp.where(is_mid, 2, 1)
    for index in range(4):
        peers = peers + goes(index).astype(jnp.int32)

        @pl.when(goes(index))
        def _():
            greet("sec", sector + OFFSETS[index])

    pl.semaphore_wait(barrier, peers)

    large[1].wait()

    @pl.when(is_mid)
    def _():
        for part in range(2):
            state_copy(0, me, part, near_end).start()
            state_copy(1, me, part, other_mid).start()

        @pl.loop(0, 2)
        def _(term):
            own_copy(term, other_mid).start()

    @pl.when(is_end)
    def _():
        for part in range(2):
            state_copy(0, me, part, near_mid).start()

        @pl.loop(0, terms)
        def _(term):
            own_copy(term, near_mid).start()

    for copy in small:
        copy.wait()
    read_channels(slots, terms, sector, term_ids, out_ids, coef, coefs, kept, filled, table)
    spots_copy = pltpu.make_async_copy(table, spots, local_sems.at[7])
    spots_copy.start()
    acc[...] = jnp.zeros_like(acc)
    acc_end[...] = jnp.zeros_like(acc_end)
    running[...] = jnp.zeros_like(running)

    live = dims[0]
    inside_col = lax.broadcasted_iota(jnp.int32, (rows, width), 1) < live

    def mask_rows(owner):
        row = lax.broadcasted_iota(jnp.int32, (rows, width), 0) + owner * rows
        spot = pl.ds(pl.multiple_of(owner * rows, rows), rows)
        masked[spot, :] = jnp.where(
            inside_col & (row < live), state_all[owner].astype(F32), 0.0
        ).astype(BF16)

    def block_of(owner, term, spot):
        return jnp.dot(
            masked[spot, :], gathered[owner, term], preferred_element_type=F32
        ).astype(BF16)

    large[2].wait()

    @pl.when(is_mid)
    def _():
        for part in range(2):
            state_copy(0, other_mid, part, me).wait_recv()
            state_copy(2, other_mid, part, near_end).start()
            state_copy(0, near_end, part, me).wait_recv()
            state_copy(3, near_end, part, other_mid).start()

        @pl.loop(2, terms)
        def _(term):
            own_copy(term, other_mid).start()

        @pl.loop(0, 3)
        def _(which):
            mask_rows(jnp.where(which == 0, me, jnp.where(which == 1, other_mid, near_end)))

        @pl.loop(0, terms)
        def _(term):
            blocks[me, term, near_rows, :] = block_of(me, term, near_rows)
            turns = jnp.logical_not(edge) & (term >= turned)

            @pl.when(turns)
            def _():
                turn_off(term).start()

            @pl.when(jnp.logical_not(turns))
            def _():
                send_block(own_send, 1, me, term)

    spots_copy.wait()
    large[0].wait()
    channels = left_all.shape[0]

    def inside(spot):
        return jnp.minimum(jnp.maximum(spot, 0), channels - 1)

    @pl.loop(0, channels)
    def _(step):
        row = pl.ds(step, 1)
        total = running[...] * kept[row, :] + left_all[inside(spots[0, step])].astype(F32) * coefs[row, :]
        running[...] = total
        summed[step] = total.astype(BF16)

    @pl.loop(0, terms)
    def _(term):
        for slot in range(slots):
            cell = term * slots + slot
            value = summed[inside(spots[1, cell])].astype(F32) * filled[pl.ds(cell, 1), :]
            comb[term, slot * rows:(slot + 1) * rows, :] = value.astype(BF16)

    @pl.when(is_end)
    def _():
        for index, slot in enumerate(END_SLOTS):
            @pl.when(goes(index))
            def _():
                @pl.loop(cut, terms)
                def _(term):
                    extra_copy(slot, term, near_mid).start()

                @pl.loop(0, groups)
                def _(group):
                    end_copy(slot, group, near_mid).start()

        @pl.loop(cut, terms)
        def _(term):
            extra_copy(home, term, near_mid).start()

        @pl.loop(0, strips)
        def _(part):
            @pl.loop(0, groups)
            def _(group):
                home_copy(part, group, near_mid).start()

    def across(index):
        return (sector // 2 + (sector + OFFSETS[index]) // 2) % 4 == 3

    def send_parts(owner):
        for index, slot in enumerate(END_SLOTS):
            stage[index, owner] = acc[owner, slot * rows:(slot + 1) * rows, :].astype(BF16)

        for first in (True, False):
            for index in range(4):
                @pl.when(goes(index) & (across(index) == first))
                def _():
                    part_copy(index, owner).start()

    def take_parts(owner):
        for index in range(4):
            @pl.when(comes(index))
            def _():
                part_copy(index, owner).wait_recv()
                acc[owner, home * rows:(home + 1) * rows, :] += landed[index, owner].astype(F32)

    def write_out(owner):
        for spot in range(4):
            @pl.when(owner == spot)
            def _():
                out_ref[:, spot * cols:(spot + 1) * cols] = acc[spot, home * rows:(home + 1) * rows, :]

    def far_blocks(owner, group):
        return jnp.concatenate(
            [blocks[owner, group * per + index, far_rows, :] for index in range(per)], axis=0
        )

    def end_rows(slot, group, spot):
        return jnp.concatenate(
            [comb_end[slot, group, index, spot, :] for index in range(per)], axis=1
        )

    def add_end(slot, owners, spot, left, rights):
        for first in range(0, len(owners), 2):
            pair = owners[first:first + 2]
            product = jnp.dot(
                left, jnp.concatenate(rights[first:first + 2], axis=1), preferred_element_type=F32
            )
            for index, owner in enumerate(pair):
                acc_end[slot, owner, spot, :] += product[:, index * cols:(index + 1) * cols]

    def end_multiply(slot, group, owners, spot=slice(None)):
        rights = [far_blocks(owner, group) for owner in owners]
        add_end(slot, owners, spot, end_rows(slot, group, spot), rights)

    extras = comb_extra.shape[1]
    has_extras = edge | (least > 0)

    def extra_left(slot):
        return jnp.concatenate([comb_extra[slot, index] for index in range(extras)], axis=1)

    def extra_right(owner):
        return jnp.concatenate(
            [blocks[owner, terms - 1 - index, extra_rows, :] for index in range(extras)], axis=0
        )

    def extra_multiply(slot, owners):
        @pl.loop(cut, terms)
        def _(term):
            extra_copy(slot, term, me).wait_recv()

        @pl.when(has_extras)
        def _():
            rights = [extra_right(owner) for owner in owners]
            add_end(slot, owners, slice(None), extra_left(slot), rights)

    def add_far(left, right):
        product = jnp.dot(
            jnp.concatenate(left, axis=0), right, preferred_element_type=F32
        )
        for index, slot in enumerate(END_SLOTS):
            acc_end[slot, far_end] += product[index * rows:(index + 1) * rows]

    def send_end_parts(index, owner):
        @pl.when(goes(index))
        def _():
            stage_end[index, owner] = acc_end[OFFSETS[index] + 2, owner].astype(BF16)
            part_end_copy(index, owner).start()

    @pl.when(is_mid)
    def _():
        def near_owner(which):
            return jnp.where(which == 0, me, jnp.where(which == 1, other_mid, near_end))

        def multiply(owner, term):
            acc[owner] += jnp.dot(comb[term], blocks[owner, term], preferred_element_type=F32)

        near_three = [me, other_mid, near_end]

        def add_far_group(group):
            add_far(
                [end_rows(slot, group, slice(None)) for slot in END_SLOTS],
                far_blocks(far_end, group),
            )

        for index, slot in enumerate(END_SLOTS):
            @pl.when(jnp.logical_not(goes(index)))
            def _():
                comb_end[slot] = jnp.zeros(comb_end.shape[1:], BF16)
                comb_extra[slot] = jnp.zeros(comb_extra.shape[1:], BF16)

        state_wait(far_end)
        mask_rows(far_end)

        @pl.when(edge)
        def _():
            @pl.loop(turned, terms)
            def _(term):
                turn_off(term).wait_recv()
                pass_on(term).start()

        @pl.loop(0, terms)
        def _(term):
            blocks[me, term, far_rows, :] = block_of(me, term, far_rows)

        everything = slice(None)

        @pl.loop(0, terms)
        def _(term):
            arrived(other_mid, term)
            blocks[other_mid, term] = block_of(other_mid, term, everything)
            send_block(relay_send, 0, other_mid, term)
            arrived(near_end, term)
            relay_copy(near_end, term, other_mid).start()
            blocks[near_end, term] = block_of(near_end, term, everything)

            @pl.loop(0, 3)
            def _(which):
                multiply(near_owner(which), term)

        @pl.loop(0, 3)
        def _(which):
            send_parts(near_owner(which))

        @pl.loop(0, terms)
        def _(term):
            arrived(far_end, term)
            blocks[far_end, term] = block_of(far_end, term, everything)
            send_block(relay_send, 2, far_end, term)

            @pl.when(term < terms - 1)
            def _():
                multiply(far_end, term)

            for index in range(4):
                slot = OFFSETS[index] + 2

                @pl.when((term == (index + 1) * terms // 4 - 2) & goes(index))
                def _():
                    extra_multiply(slot, near_three)

                    @pl.loop(0, groups)
                    def _(group):
                        end_copy(slot, group, me).wait_recv()

                        end_multiply(slot, group, near_three)

                    @pl.loop(0, 3)
                    def _(which):
                        send_end_parts(index, near_owner(which))

            @pl.when(term == terms - 2)
            def _():
                @pl.loop(0, groups - 1)
                def _(group):
                    add_far_group(group)

        add_far_group(groups - 1)

        @pl.when(has_extras)
        def _():
            add_far([extra_left(slot) for slot in END_SLOTS], extra_right(far_end))

        for index, slot in enumerate(END_SLOTS):
            stage_end[index, far_end] = acc_end[slot, far_end].astype(BF16)

        for first in (True, False):
            for index in range(4):
                @pl.when(goes(index) & (across(index) == first))
                def _():
                    part_end_copy(index, far_end).start()

        multiply(far_end, terms - 1)

        extra_multiply(home, [0, 1, 2, 3])

        def home_strip(part):
            @pl.loop(0, groups)
            def _(group):
                home_copy(part, group, me).wait_recv()

                spot = pl.ds(pl.multiple_of(part * strip, strip), strip)
                end_multiply(home, group, [0, 1, 2, 3], spot)

        def send_back(part):
            spot = pl.ds(pl.multiple_of(part * strip, strip), strip)
            back[:, spot, :] = acc_end[home, :, spot, :].astype(BF16)
            back_copy(part, near_end).start()

        def take_end_parts(owner):
            for index in range(4):
                @pl.when(comes(index))
                def _():
                    part_end_copy(index, owner).wait_recv()
                    acc_end[home, owner] += landed_end[index, owner].astype(F32)

        @pl.loop(0, 3)
        def _(which):
            take_end_parts(near_owner(which))

        home_strip(0)
        take_end_parts(far_end)
        send_back(0)
        send_parts(far_end)

        @pl.loop(1, strips)
        def _(part):
            home_strip(part)
            send_back(part)

        @pl.loop(0, 4)
        def _(owner):
            take_parts(owner)
            write_out(owner)

    @pl.when(is_end)
    def _():
        turn = jnp.where(me == 0, 1, -1)
        state_wait(near_mid)
        state_wait(3 - near_mid)

        @pl.loop(0, 3)
        def _(rank):
            mask_rows(me + turn * rank)

        def multiply(owner, term, block, spot):
            acc[owner] += jnp.dot(comb[term, :, spot], block, preferred_element_type=F32)

        @pl.loop(0, cut)
        def _(term):
            multiply(me, term, block_of(me, term, near_rows), near_rows)

        @pl.loop(cut, terms)
        def _(term):
            multiply(me, term, block_of(me, term, short_rows), short_rows)

        send_parts(me)

        @pl.loop(1, 4)
        def _(rank):
            owner = me + turn * rank

            @pl.loop(0, cut)
            def _(term):
                block_arrived(owner, term, near_rows)
                multiply(owner, term, blocks[owner, term, near_rows, :], near_rows)

            @pl.loop(cut, terms)
            def _(term):
                block_arrived(owner, term, short_rows)
                multiply(owner, term, blocks[owner, term, short_rows, :], short_rows)

            send_parts(owner)

        @pl.loop(0, 3)
        def _(rank):
            take_parts(me + turn * rank)

        @pl.loop(0, strips)
        def _(part):
            back_copy(part, me).wait_recv()

        acc[:, home * rows:(home + 1) * rows, :] += back_landed[...].astype(F32)

        @pl.loop(0, 3)
        def _(rank):
            write_out(me + turn * rank)

        take_parts(far_end)
        write_out(far_end)

    for index in range(4):
        @pl.when(goes(index))
        def _():
            @pl.loop(0, 4)
            def _(owner):
                part_copy(index, owner).wait_send()

                @pl.when(is_mid)
                def _():
                    part_end_copy(index, owner).wait_send()

    @pl.when(is_mid)
    def _():
        for part in range(2):
            state_copy(0, me, part, near_end).wait_send()
            state_copy(1, me, part, other_mid).wait_send()
            state_copy(2, other_mid, part, near_end).wait_send()
            state_copy(3, near_end, part, other_mid).wait_send()

        @pl.loop(0, terms)
        def _(term):
            own_copy(term, other_mid).wait_send()
            relay_copy(near_end, term, other_mid).wait_send()
            turns = jnp.logical_not(edge) & (term >= turned)

            @pl.when(turns)
            def _():
                turn_off(term).wait_send()

            @pl.when(edge & (term >= turned))
            def _():
                pass_on(term).wait_send()

            @pl.when(jnp.logical_not(turns))
            def _():
                sent_block(own_send, 1, me, term)

            sent_block(relay_send, 0, other_mid, term)
            sent_block(relay_send, 2, far_end, term)

        @pl.loop(0, strips)
        def _(part):
            back_copy(part, near_end).wait_send()

    @pl.when(is_end)
    def _():
        for part in range(2):
            state_copy(0, me, part, near_mid).wait_send()

        @pl.loop(0, terms)
        def _(term):
            own_copy(term, near_mid).wait_send()

        for index, slot in enumerate(END_SLOTS):
            @pl.when(goes(index))
            def _():
                @pl.loop(cut, terms)
                def _(term):
                    extra_copy(slot, term, near_mid).wait_send()

                @pl.loop(0, groups)
                def _(group):
                    end_copy(slot, group, near_mid).wait_send()

        @pl.loop(cut, terms)
        def _(term):
            extra_copy(home, term, near_mid).wait_send()

        @pl.loop(0, strips)
        def _(part):
            @pl.loop(0, groups)
            def _(group):
                home_copy(part, group, near_mid).wait_send()


def line_apply(sectors, slots, dims, channel_term, channel_out, coefs, state, right, left):
    terms, width, cols = right.shape
    rows = state.shape[0]
    channels = left.shape[0]
    cells = slots * terms
    per = 4
    groups = terms // per
    strips = 2
    detours, extras, least = (3, 6, 0) if sectors == 8 and terms == 16 else (0, 1, 1)
    tall = slots * rows
    dma = pltpu.SemaphoreType.DMA
    any_space = pl.BlockSpec(memory_space=pl.ANY)
    return pl.pallas_call(
        functools.partial(line_kernel, sectors, detours, least),
        out_shape=pltpu.VMEM((rows, width), F32),
        in_specs=[any_space] * 7,
        out_specs=pl.BlockSpec(memory_space=pltpu.VMEM),
        scratch_shapes=[
            pltpu.SMEM(dims.shape, jnp.int32),
            pltpu.VMEM((channels,), jnp.int32),
            pltpu.VMEM((channels,), jnp.int32),
            pltpu.VMEM((channels,), BF16),
            pltpu.VMEM((8, 128), jnp.int32),
            pltpu.SMEM((8, 128), jnp.int32),
            pltpu.VMEM((channels, width), F32),
            pltpu.VMEM((channels, width), F32),
            pltpu.VMEM((cells, width), F32),
            pltpu.VMEM(left.shape, BF16),
            pltpu.VMEM((rows, width), F32),
            pltpu.VMEM(left.shape, BF16),
            pltpu.VMEM((4, rows, width), BF16),
            pltpu.VMEM((width, width), BF16),
            pltpu.VMEM((4, terms, width, cols), BF16),
            pltpu.VMEM((4, terms, width, cols), BF16),
            pltpu.VMEM((terms, tall, width), BF16),
            pltpu.VMEM((slots, groups, per, rows, rows), BF16),
            pltpu.VMEM((slots, extras, rows, rows), BF16),
            pltpu.VMEM((max(detours, 1), width - rows, cols), BF16),
            pltpu.VMEM((4, tall, cols), F32),
            pltpu.VMEM((slots, 4, rows, cols), F32),
            pltpu.VMEM((4, 4, rows, cols), BF16),
            pltpu.VMEM((4, 4, rows, cols), BF16),
            pltpu.VMEM((4, 4, rows, cols), BF16),
            pltpu.VMEM((4, 4, rows, cols), BF16),
            pltpu.VMEM((4, rows, cols), BF16),
            pltpu.VMEM((4, rows, cols), BF16),
            dma((8,)), dma((4, 2)), dma((4, 2)),
            dma((2, terms)), dma((3, terms)), dma((4, terms)),
            dma((slots, groups)), dma((slots, groups)), dma((slots, extras)), dma((slots, extras)),
            dma((strips, groups)), dma((strips, groups)),
            dma((2, max(detours, 1))), dma((max(detours, 1),)),
            dma((4, 4)), dma((4, 4)), dma((4, 4)), dma((4, 4)), dma((2, strips)),
        ],
        compiler_params=pltpu.CompilerParams(
            has_side_effects=True, collective_id=0, vmem_limit_bytes=60 * 2**20
        ),
    )(dims, channel_term, channel_out, coefs, state, right, left)


def passed_along(value, axis, steps):
    count = lax.axis_size(axis)
    first, last = (max(0, -steps), min(count, count - steps))
    return lax.ppermute(value, axis, [(source, source + steps) for source in range(first, last)])


def gathered_apply(sector, live_dim, wave, right, combined, rows, slots):
    width = wave.shape[1]
    terms = right.shape[0]
    whole_state = lax.all_gather(wave, "pan", axis=0, tiled=True)
    indices = lax.iota(jnp.int32, width)
    inside = (indices[:, None] < live_dim) & (indices[None, :] < live_dim)
    masked = jnp.where(inside, whole_state, jnp.zeros((), BF16))
    right_full = lax.all_gather(right, "pan", axis=2, tiled=True)
    term_full = jnp.einsum("ik,wkq->wiq", masked, right_full, preferred_element_type=F32).astype(BF16)
    parts = jnp.einsum(
        "wjri,wiq->jrq", combined.reshape(terms, slots, rows, width), term_full,
        preferred_element_type=F32,
    )
    collected = parts[2]
    for offset in OFFSETS:
        collected = collected + passed_along(parts[offset + 2], "sec", offset)
    return collected


def on_device(
    wave_state, right_blocks, left_blocks, coupling, channel_term, channel_out, sector_dims
):
    rows, width = wave_state.shape[1:]
    terms = right_blocks.shape[1]
    slots = 5
    sector = lax.axis_index("sec")
    live_dim = sector_dims[0]
    if lax.axis_size("pan") == 4 and right_blocks.shape[3] % 128 == 0 and terms % 4 == 0:
        collected = line_apply(
            lax.axis_size("sec"), slots, sector_dims, channel_term, channel_out, coupling,
            wave_state[0], right_blocks[0], left_blocks,
        )
    else:
        cells = channel_term * slots + channel_out - sector + 2
        coefs = coupling.astype(F32)
        combined = combine(cells, coefs, left_blocks, terms * slots)
        collected = gathered_apply(
            sector, live_dim, wave_state[0], right_blocks[0], combined, rows, slots
        )
    indices = lax.iota(jnp.int32, width)
    row_ids = lax.axis_index("pan") * rows + lax.iota(jnp.int32, rows)
    kept_mask = (row_ids[:, None] < live_dim) & (indices[None, :] < live_dim)
    return jnp.where(kept_mask, collected, jnp.zeros((), F32))[None]


def solution(mesh):
    return jax.shard_map(
        on_device,
        mesh=mesh,
        in_specs=(
            P("sec", "pan", None),
            P("sec", None, None, "pan"),
            P("sec", "pan", None),
            P("sec"),
            P("sec"),
            P("sec"),
            P("sec"),
        ),
        out_specs=P("sec", "pan", None),
        check_vma=False,
    )
```
